256 devices in a mesh: row: 32 (over y, z), col: 8 (over x, core).
Axes of the slice: x: 4, y: 4, z: 8, core: 2. Of those that a mesh axis runs over, the one named last changes fastest.
Arguments:
- eigvec: float32 [8, 32, 128, 2048], P(None, 'row', None, 'col'), may hold values from -6 to 6
- reflectors: float32 [2, 8, 32, 256, 128], P(None, None, 'row', 'col'), may hold values from -6 to 6
- sweep_group: int32 [2, 8, 32], P(None, None, 'row'), may hold values from -1 to 254, as said below
Outputs:
- transformed: float32 [8, 32, 128, 2048], P(None, 'row', None, 'col')
The draws below stay inside these ranges and needn't reach their ends.
Inputs may be any that keep to these rules, and one draw needn't show every extreme that they name: `sweep_group`: -1 where no diamond sits at that diagonal and tile position (tile position l * R + r for entry [d, l, r]); otherwise the diamond's sweep group, at most its tile position. Within one diagonal no two diamonds sit at adjacent tile positions, and none sits at the last tile position 255.
All inputs are finite; a program needn't handle non-finite values.
Results may differ from the reference program's by a relative error of at most 0.0003.
Values sent between devices are 32-bit elements.
A program may use at most 128 MiB of HBM per device.

```python
import jax
import jax.numpy as jnp
from jax import lax

B = 128
DIAG = 2
NT = 256
TILES_DEV = 8
NC = 2048
N_ROW = 32


def draw_sweep_group(key, part):
    first_key = jax.random.fold_in(key, 11)
    second_key = jax.random.fold_in(key, 12)
    bits = jax.random.randint(first_key, (DIAG, NT), 0, 2).astype(jnp.int32)
    earlier = jnp.concatenate([jnp.zeros((DIAG, 1), jnp.int32), bits[:, :-1]], axis=1)
    positions = jnp.broadcast_to(jnp.arange(NT, dtype=jnp.int32)[None, :], (DIAG, NT))
    present = (bits == 1) & (earlier == 0) & (positions < NT - 1)
    groups = jax.random.randint(second_key, (DIAG, NT), 0, positions + 1).astype(jnp.int32)
    result = jnp.where(present, groups, -jnp.ones_like(groups))
    return result.reshape(DIAG, TILES_DEV, NT // TILES_DEV).astype(jnp.int32)


def level_of(key, dims, shards, least, largest):
    def one(dim, shards_of):
        steps = jax.random.uniform(jax.random.fold_in(jax.random.fold_in(key, 6), dim), (shards_of,), jnp.float32, least / len(shards), largest / len(shards))
        return jnp.repeat(jnp.exp(steps), dims[dim] // shards_of).reshape((-1,) + (1,) * (len(dims) - dim - 1))

    factor_of = one(*shards[0])
    for cut in shards[1:]:
        factor_of = factor_of * one(*cut)
    return factor_of


def gaussian(key, shape, deviation, reach, shards=(), kind=jnp.bfloat16):
    values = deviation * jax.random.normal(key, shape, jnp.float32)
    if shards:
        values = values * level_of(key, shape, shards, -0.22, 0.18)
    return jnp.clip(values, -reach, reach).astype(kind)


def setup_inputs(seed: int = 0) -> dict:
    streams_of = jax.random.split(jax.random.key(seed), 4)
    return {
        "eigvec": gaussian(streams_of[0], (TILES_DEV, N_ROW, B, NC), 1.0, 6.0, ((1, 32), (3, 8)), jnp.float32),
        "reflectors": gaussian(streams_of[1], (DIAG, TILES_DEV, N_ROW, 2 * B, B), 1.0, 6.0, ((2, 32), (3, 8)), jnp.float32),
        "sweep_group": draw_sweep_group(jax.random.fold_in(streams_of[3], 71), 0),
    }


highest_mode = lax.Precision.HIGHEST


def masked_vectors(panels):
    depth_rows = panels.shape[-2]
    band_width = panels.shape[-1]
    row_iota = lax.broadcasted_iota(jnp.int32, (depth_rows, band_width), 0)
    col_iota = lax.broadcasted_iota(jnp.int32, (depth_rows, band_width), 1)
    inside = (row_iota >= col_iota + 1) & (row_iota <= col_iota + band_width)
    leading = row_iota == col_iota + 1
    kept = jnp.where(inside, panels, jnp.zeros_like(panels))
    return jnp.where(leading, jnp.ones_like(panels), kept)


def inverse_factor(vectors):
    band_width = vectors.shape[-1]
    gram_matrix = jnp.einsum("...ji,...jk->...ik", vectors, vectors, precision=highest_mode)
    diagonal_part = jnp.diagonal(gram_matrix, axis1=-2, axis2=-1)
    strict_upper = jnp.triu(gram_matrix, 1)
    return strict_upper + jnp.eye(band_width, dtype=vectors.dtype) * (0.5 * diagonal_part[..., None, :])


def invert_upper(factor):
    band_width = factor.shape[-1]
    row_iota = lax.broadcasted_iota(jnp.int32, (band_width, band_width), 0)
    col_iota = lax.broadcasted_iota(jnp.int32, (band_width, band_width), 1)
    diagonal_part = jnp.diagonal(factor, axis1=-2, axis2=-1)
    eye_matrix = (row_iota == col_iota).astype(factor.dtype)
    inverse = eye_matrix * (1.0 / diagonal_part)[..., None, :]
    block = 1
    while block < band_width:
        coupling = ((row_iota // block) != (col_iota // block)) & ((row_iota // (2 * block)) == (col_iota // (2 * block)))
        upper_part = jnp.where(coupling, factor, jnp.zeros_like(factor))
        middle = jnp.einsum("...ij,...jk->...ik", upper_part, inverse, precision=highest_mode)
        inverse = inverse - jnp.einsum("...ij,...jk->...ik", inverse, middle, precision=highest_mode)
        block = block * 2
    return inverse


def reflect(stacked, vectors, factor):
    weights = jnp.einsum("...ji,...jc->...ic", vectors, stacked, precision=highest_mode)
    solved = jnp.einsum("...ik,...kc->...ic", invert_upper(factor), weights, precision=highest_mode)
    return stacked - jnp.einsum("...ji,...ic->...jc", vectors, solved, precision=highest_mode)


def apply_one(item):
    stacked, panels, flag = item
    vectors = masked_vectors(panels)
    factor = inverse_factor(vectors)
    updated = reflect(stacked, vectors, factor)
    return jnp.where(flag >= 0, updated, stacked)


def reference(eigvec, reflectors, sweep_group):
    tiles_dev = eigvec.shape[0]
    cycle_size = eigvec.shape[1]
    band = eigvec.shape[2]
    columns = eigvec.shape[3]
    total = tiles_dev * cycle_size
    diagonals = reflectors.shape[0]
    current = eigvec.reshape(total, band, columns)
    panels_all = reflectors.reshape(diagonals, total, 2 * band, band)
    flags_all = sweep_group.reshape(diagonals, total)
    for diagonal in range(diagonals):
        stacked = current.reshape(total // 2, 2 * band, columns)
        updated = lax.map(apply_one, (stacked, panels_all[diagonal, 0::2], flags_all[diagonal, 0::2]))
        current = updated.reshape(total, band, columns)
        inner = current[1:total - 1].reshape(total // 2 - 1, 2 * band, columns)
        updated = lax.map(apply_one, (inner, panels_all[diagonal, 1:total - 1:2], flags_all[diagonal, 1:total - 1:2]))
        current = jnp.concatenate([current[:1], updated.reshape(total - 2, band, columns), current[total - 1:]], axis=0)
    return current.reshape(tiles_dev, cycle_size, band, columns)
```

```python
import jax
import jax.numpy as jnp
from jax import lax
from jax.experimental import pallas as pl
from jax.experimental.pallas import tpu as pltpu
from jax.sharding import PartitionSpec as P

MESH = pl.DeviceIdType.MESH
f32, bf16 = jnp.float32, jnp.bfloat16


def split(a):
    hi = a.astype(bf16)
    return hi, (a - hi.astype(f32)).astype(bf16)


def mm(a, b):
    return jnp.dot(a, b, preferred_element_type=f32)


def square_dot(a, b):
    n = a.shape[-1]
    a_hi, a_lo = split(a)
    b_hi, b_lo = split(b)
    right = jnp.concatenate([b_hi, b_lo], axis=1)
    both = mm(jnp.concatenate([a_hi, a_lo], axis=1), jnp.concatenate([right, right], axis=0))
    return both[:, :n] + both[:, n:]


def factor_panels(panels):
    depth, band = panels[0].shape
    rows = lax.broadcasted_iota(jnp.int32, (depth, band), 0)
    cols = lax.broadcasted_iota(jnp.int32, (depth, band), 1)
    inside = (rows >= cols + 1) & (rows <= cols + band)
    leading = rows == cols + 1
    r = lax.broadcasted_iota(jnp.int32, (band, band), 0)
    c = lax.broadcasted_iota(jnp.int32, (band, band), 1)
    eye, above = r == c, r < c
    halves, turned, factors, inverses = [], [], [], []
    for panel in panels:
        vectors = jnp.where(leading, 1.0, jnp.where(inside, panel, 0.0))
        v_hi, v_lo = split(vectors)
        t_hi, t_lo = split(vectors.T)
        both = mm(t_hi, jnp.concatenate([v_hi, v_lo], axis=1))
        gram = both[:, :band] + both[:, band:] + mm(t_lo, v_hi)
        on_diagonal = jnp.where(eye, gram, 0.0)
        along = 2.0 / jnp.sum(on_diagonal, axis=0, keepdims=True)
        down = 2.0 / jnp.sum(on_diagonal, axis=1, keepdims=True)
        pair = above & (r // 2 == c // 2)
        inverse = jnp.where(eye, along, 0.0) - jnp.where(pair, gram * along * down, 0.0)
        halves.append((v_hi, v_lo))
        turned.append((t_hi, t_lo))
        factors.append(gram)
        inverses.append(inverse)
    block = 2
    while block < band:
        coupling = above & (r // block != c // block) & (r // (2 * block) == c // (2 * block))
        middles = [square_dot(jnp.where(coupling, f, 0.0), x) for f, x in zip(factors, inverses)]
        inverses = [x - square_dot(x, m) for x, m in zip(inverses, middles)]
        block *= 2
    results = []
    for (v_hi, v_lo), (t_hi, t_lo), inverse in zip(halves, turned, inverses):
        i_hi, i_lo = split(inverse)
        solver = mm(jnp.concatenate([i_hi, i_lo], axis=1), jnp.concatenate([t_hi, t_hi], axis=0)) + mm(i_hi, t_lo)
        p_hi, p_lo = split(solver)
        results.append((v_hi, v_lo, p_hi, p_lo))
    return results


def kernel(n_row, n_x, eig, refl, flags, out,
           xin, xb, xs, xf, xq, xc, u1, us, u2, s1, ss, s2, d1, ds, d2, pan, vv, pp,
           in_sem, pan_in, pan_send, pan_recv, rel_send, rel_recv,
           up_send, up_recv, dn_send, dn_recv, out_sem):
    row = lax.axis_index("row")
    col = lax.axis_index("col")
    band = xin.shape[1]
    per = pan.shape[2]
    x, core = col // 2, lax.rem(col, 2)
    first = row == 0
    last = row == n_row - 1
    shift = jnp.where(first, 1, 0)
    above = lax.rem(row + n_row - 1, n_row)
    below = lax.rem(row + 1, n_row)
    twice0 = jnp.where(lax.rem(row, 2) == 1, 0, per)
    once0 = per - twice0
    partner = x * 2 + (1 - core)
    peers = [lax.rem(x + k, n_x) * 2 + core for k in range(1, n_x)]

    chunk_of = ((0, twice0), (0, once0), (1, once0), (1, twice0))
    tiles_in = pltpu.make_async_copy(eig.at[:, 0], xin, in_sem)
    tiles_in.start()
    panels_in = []
    for k, (d, l0) in enumerate(chunk_of):
        copy = pltpu.make_async_copy(refl.at[d, pl.ds(l0, per), 0], pan.at[k, col], pan_in.at[k])
        copy.start()
        panels_in.append(copy)

    barrier = pltpu.get_barrier_semaphore()
    for r_, c_ in [(above, col), (below, col), (row, partner)] + [(row, p) for p in peers]:
        pl.semaphore_signal(barrier, inc=1, device_id=(r_, c_), device_id_type=MESH)
    pl.semaphore_wait(barrier, 3 + len(peers))

    def remote(src, dst, ssem, rsem, r_, c_):
        return pltpu.make_async_remote_copy(src_ref=src, dst_ref=dst, send_sem=ssem, recv_sem=rsem,
                                            device_id=(r_, c_), device_id_type=MESH)

    def upward(kind, src, dst, i):
        return remote(src, dst.at[i], up_send.at[kind, i], up_recv.at[kind, i], above, col)

    def downward(kind, src, dst, i):
        return remote(src, dst.at[i], dn_send.at[kind, i], dn_recv.at[kind, i], below, col)

    def share(k, j):
        return remote(pan.at[k, col], pan.at[k, col], pan_send.at[k, j], pan_recv.at[k, j],
                      row, partner if j == n_x - 1 else peers[j])

    def came(k, j):
        origin = partner if j == n_x - 1 else lax.rem(x + n_x - 1 - j, n_x) * 2 + core
        return remote(pan.at[k, origin], pan.at[k, origin], pan_send.at[k, j], pan_recv.at[k, j], row, partner)

    def passed(k, j):
        origin = lax.rem(x + n_x - 1 - j, n_x) * 2 + core
        return remote(pan.at[k, origin], pan.at[k, origin], rel_send.at[k, j], rel_recv.at[k, j], row, partner)

    def passed_here(k, j):
        origin = lax.rem(x + n_x - 1 - j, n_x) * 2 + (1 - core)
        return remote(pan.at[k, origin], pan.at[k, origin], rel_send.at[k, j], rel_recv.at[k, j], row, partner)

    order = [0, n_x - 2] + list(range(1, n_x - 2))
    panels_in[0].wait()
    for j in order + [n_x - 1]:
        share(0, j).start()
    tiles_in.wait()
    for i in range(per):
        upward(0, xin.at[once0 + i + shift], u1, i).start()
    for k in range(1, 4):
        panels_in[k].wait()
        for j in order + [n_x - 1]:
            share(k, j).start()

    def pass_on(k):
        for j in order:
            came(k, j).wait_recv()
            passed(k, j).start()

    def settle(k):
        came(k, n_x - 1).wait_recv()
        for j in order:
            passed_here(k, j).wait_recv()

    def factor_chunk(k):
        raw = [pan[k, :, i].reshape(2 * band, band) for i in range(per)]
        for i, (v_hi, v_lo, p_hi, p_lo) in enumerate(factor_panels(raw)):
            vv[k, i, 0] = v_hi
            vv[k, i, 1] = v_lo
            pp[k, i, 0] = p_hi
            pp[k, i, 1] = p_lo

    def apply(k, i, d, l, upper, lower):
        s_hi, s_lo = split(jnp.concatenate([upper, lower], axis=0))
        p_hi, p_lo = pp[k, i, 0], pp[k, i, 1]
        v_hi, v_lo = vv[k, i, 0], vv[k, i, 1]
        w_hi, w_lo = split(mm(p_hi, s_hi) + mm(p_hi, s_lo) + mm(p_lo, s_hi))
        change = mm(jnp.concatenate([v_hi, v_lo], axis=1), jnp.concatenate([w_hi, w_hi], axis=0)) + mm(v_hi, w_lo)
        active = flags[d, l, 0] >= 0
        return (jnp.where(active, upper - change[:band], upper), jnp.where(active, lower - change[band:], lower))

    pass_on(0)
    settle(0)
    factor_chunk(0)
    pass_on(1)

    def early(i, carry):
        l = twice0 + i
        upward(0, u1.at[i], u1, i).wait_recv()
        upper, lower = apply(0, i, 0, l, xin[l], u1[i])
        s1[i] = lower
        xb[i] = upper
        downward(0, s1.at[i], d1, i).start()

        @pl.when(jnp.logical_not(first))
        def _():
            upward(1, xb.at[i], us, i).start()

        @pl.when(first & (i > 0))
        def _():
            upward(1, xb.at[i], us, i - 1).start()

        return carry

    lax.fori_loop(0, per, early, 0)

    @pl.when(first)
    def _():
        upward(1, xb.at[per - 1], us, per - 1).start()

    settle(1)
    pass_on(2)
    factor_chunk(1)
    settle(2)
    pass_on(3)
    factor_chunk(2)

    def middle(i, carry):
        l = once0 + i

        @pl.when(first & (i == 0))
        def _():
            xq[...] = xin[once0]

        @pl.when(jnp.logical_not(first & (i == 0)))
        def _():
            j = i - shift
            downward(0, d1.at[j], d1, j).wait_recv()
            xq[...] = d1[j]

        upward(1, us.at[i], us, i).wait_recv()
        upper, lower = apply(1, i, 0, l, xq[...], us[i])
        upper, lower = apply(2, i, 1, l, upper, lower)
        ss[i] = lower
        xs[i] = upper
        downward(1, ss.at[i], ds, i).start()

        @pl.when(jnp.logical_not(first & (i == 0)))
        def _():
            upward(2, xs.at[i], u2, i - shift).start()

        return carry

    lax.fori_loop(0, per, middle, 0)
    settle(3)
    factor_chunk(3)

    @pl.when(first)
    def _():
        downward(0, d1.at[per - 1], d1, per - 1).wait_recv()
        xq[...] = jnp.where(flags[0, twice0, 0] >= 0, xb[0], d1[per - 1])
        upward(2, xq, u2, per - 1).start()

    def late(i, carry):
        l = twice0 + i

        @pl.when(jnp.logical_not(first & (i == 0)))
        def _():
            j = i - shift
            downward(1, ds.at[j], ds, j).wait_recv()

            xc[...] = ds[j]

        @pl.when(first & (i == 0))
        def _():
            xc[...] = xq[...]
            downward(1, ds.at[per - 1], ds, per - 1).wait_recv()

        upward(2, u2.at[i], u2, i).wait_recv()
        upper, lower = apply(3, i, 1, l, xc[...], u2[i])
        s2[i] = lower
        xf[i] = upper
        downward(2, s2.at[i], d2, i).start()

        @pl.when(jnp.logical_not(first & (i == 0)))
        def _():
            pltpu.make_async_copy(xf.at[i], out.at[l, 0], out_sem.at[i]).start()

        return carry

    lax.fori_loop(0, per, late, 0)

    def close(i, carry):
        @pl.when(jnp.logical_not(first & (i == 0)))
        def _():
            j = i - shift
            downward(2, d2.at[j], d2, j).wait_recv()
            pltpu.make_async_copy(d2.at[j], out.at[once0 + i, 0], out_sem.at[per + i]).start()

        @pl.when(first & (i == 0))
        def _():
            pltpu.make_async_copy(xs.at[i], out.at[once0 + i, 0], out_sem.at[per + i]).start()

        return carry

    lax.fori_loop(0, per, close, 0)

    @pl.when(first)
    def _():
        downward(2, d2.at[per - 1], d2, per - 1).wait_recv()
        xq2 = jnp.where(flags[1, twice0, 0] >= 0, xf[0], d2[per - 1])
        xb[0] = xq2
        pltpu.make_async_copy(xb.at[0], out.at[twice0, 0], out_sem.at[0]).start()

    def drain(i, carry):
        for kind in range(3):
            upward(kind, xb.at[i], u1, i).wait_send()
            downward(kind, xb.at[i], d1, i).wait_send()
        pltpu.make_async_copy(xf.at[i], out.at[twice0 + i, 0], out_sem.at[i]).wait()
        pltpu.make_async_copy(xf.at[i], out.at[once0 + i, 0], out_sem.at[per + i]).wait()
        for j in range(n_x):
            share(i, j).wait_send()
        for j in range(n_x - 1):
            passed(i, j).wait_send()
        return carry

    lax.fori_loop(0, 4, drain, 0)


def local(n_row, n_x, eigvec, reflectors, sweep_group):
    tiles, _, band, width = eigvec.shape
    rows = reflectors.shape[3]
    per = tiles // 2
    tile = pltpu.VMEM((per, band, width), f32)
    dma = pltpu.SemaphoreType.DMA
    import functools
    return pl.pallas_call(
        functools.partial(kernel, n_row, n_x),
        out_shape=jax.ShapeDtypeStruct(eigvec.shape, f32),
        in_specs=[pl.BlockSpec(memory_space=pl.ANY), pl.BlockSpec(memory_space=pl.ANY),
                  pl.BlockSpec(memory_space=pltpu.SMEM)],
        out_specs=pl.BlockSpec(memory_space=pl.ANY),
        scratch_shapes=[
            pltpu.VMEM((tiles, band, width), f32),
            tile, tile, tile, pltpu.VMEM((band, width), f32), pltpu.VMEM((band, width), f32),
            tile, tile, tile, tile, tile, tile, tile, tile, tile,
            pltpu.VMEM((4, 2 * n_x, per, rows, band), f32),
            pltpu.VMEM((4, per, 2, 2 * band, band), bf16),
            pltpu.VMEM((4, per, 2, band, 2 * band), bf16),
            dma, dma((4,)), dma((4, n_x)), dma((4, n_x)), dma((4, n_x - 1)), dma((4, n_x - 1)),
            dma((3, per)), dma((3, per)), dma((3, per)), dma((3, per)), dma((2 * per,)),
        ],
        compiler_params=pltpu.CompilerParams(
            collective_id=0, has_side_effects=True, vmem_limit_bytes=48 * 1024 * 1024),
    )(eigvec, reflectors, sweep_group)


def solution(mesh):
    import functools
    return jax.shard_map(
        functools.partial(local, mesh.shape["row"], mesh.shape["col"] // 2),
        mesh=mesh,
        in_specs=(
            P(None, "row", None, "col"),
            P(None, None, "row", "col", None),
            P(None, None, "row"),
        ),
        out_specs=P(None, "row", None, "col"),
        check_vma=False,
    )
```

```python
import functools

import jax
import jax.numpy as jnp
from jax import lax
from jax.experimental import pallas as pl
from jax.experimental.pallas import tpu as pltpu
from jax.sharding import PartitionSpec as P

MESH = pl.DeviceIdType.MESH
f32, bf16 = jnp.float32, jnp.bfloat16


def split(a):
    hi = a.astype(bf16)
    return hi, (a - hi.astype(f32)).astype(bf16)


def mm(a, b):
    return jnp.dot(a, b, preferred_element_type=f32)


def square_dot(a, b):
    n = a.shape[-1]
    a_hi, a_lo = split(a)
    b_hi, b_lo = split(b)
    right = jnp.concatenate([b_hi, b_lo], axis=1)
    both = mm(jnp.concatenate([a_hi, a_lo], axis=1), jnp.concatenate([right, right], axis=0))
    return both[:, :n] + both[:, n:]


def factor_panels(panels):
    depth, band = panels[0].shape
    rows = lax.broadcasted_iota(jnp.int32, (depth, band), 0)
    cols = lax.broadcasted_iota(jnp.int32, (depth, band), 1)
    inside = (rows >= cols + 1) & (rows <= cols + band)
    leading = rows == cols + 1
    r = lax.broadcasted_iota(jnp.int32, (band, band), 0)
    c = lax.broadcasted_iota(jnp.int32, (band, band), 1)
    eye, above = r == c, r < c
    halves, turned, factors, inverses = [], [], [], []
    for panel in panels:
        vectors = jnp.where(leading, 1.0, jnp.where(inside, panel, 0.0))
        v_hi, v_lo = split(vectors)
        t_hi, t_lo = split(vectors.T)
        both = mm(t_hi, jnp.concatenate([v_hi, v_lo], axis=1))
        gram = both[:, :band] + both[:, band:] + mm(t_lo, v_hi)
        on_diagonal = jnp.where(eye, gram, 0.0)
        along = 2.0 / jnp.sum(on_diagonal, axis=0, keepdims=True)
        down = 2.0 / jnp.sum(on_diagonal, axis=1, keepdims=True)
        pair = above & (r // 2 == c // 2)
        inverse = jnp.where(eye, along, 0.0) - jnp.where(pair, gram * along * down, 0.0)
        halves.append((v_hi, v_lo))
        turned.append((t_hi, t_lo))
        factors.append(gram)
        inverses.append(inverse)
    block = 2
    while block < band:
        coupling = above & (r // block != c // block) & (r // (2 * block) == c // (2 * block))
        middles = [square_dot(jnp.where(coupling, f, 0.0), x) for f, x in zip(factors, inverses)]
        inverses = [x - square_dot(x, m) for x, m in zip(inverses, middles)]
        block *= 2
    results = []
    for (v_hi, v_lo), (t_hi, t_lo), inverse in zip(halves, turned, inverses):
        i_hi, i_lo = split(inverse)
        solver = mm(jnp.concatenate([i_hi, i_lo], axis=1), jnp.concatenate([t_hi, t_hi], axis=0)) + mm(i_hi, t_lo)
        p_hi, p_lo = split(solver)
        results.append((v_hi, v_lo, p_hi, p_lo))
    return results


def kernel(n_row, n_x, eig, refl, flags_in, out,
           flags, xin, xb, xs, xf, xq, xc, u1, us, u2, s1, ss, s2, d1, ds, d2, pan, vv, pp,
           flag_sem, in_sem, pan_in, pan_send, pan_recv, rel_send, rel_recv,
           up_send, up_recv, dn_send, dn_recv, out_sem):
    row = lax.axis_index("row")
    col = lax.axis_index("col")
    band = xin.shape[1]
    per = pan.shape[2]
    x, core = col // 2, lax.rem(col, 2)
    first = row == 0
    last = row == n_row - 1
    shift = jnp.where(first, 1, 0)
    above = lax.rem(row + n_row - 1, n_row)
    below = lax.rem(row + 1, n_row)
    twice0 = jnp.where(lax.rem(row, 2) == 1, 0, per)
    once0 = per - twice0
    partner = x * 2 + (1 - core)
    peers = [lax.rem(x + k, n_x) * 2 + core for k in range(1, n_x)]

    chunk_of = ((0, twice0), (0, once0), (1, once0), (1, twice0))
    tiles_in = pltpu.make_async_copy(eig.at[:, 0], xin, in_sem)
    tiles_in.start()
    flags_copy = pltpu.make_async_copy(flags_in, flags, flag_sem)
    flags_copy.start()
    panels_in = []
    for k, (d, l0) in enumerate(chunk_of):
        copy = pltpu.make_async_copy(refl.at[d, pl.ds(l0, per), 0], pan.at[k, col], pan_in.at[k])
        copy.start()
        panels_in.append(copy)

    barrier = pltpu.get_barrier_semaphore()
    for r_, c_ in [(above, col), (below, col), (row, partner)] + [(row, p) for p in peers]:
        pl.semaphore_signal(barrier, inc=1, device_id=(r_, c_), device_id_type=MESH)
    pl.semaphore_wait(barrier, 3 + len(peers))

    def remote(src, dst, ssem, rsem, r_, c_):
        return pltpu.make_async_remote_copy(src_ref=src, dst_ref=dst, send_sem=ssem, recv_sem=rsem,
                                            device_id=(r_, c_), device_id_type=MESH)

    def upward(kind, src, dst, i):
        return remote(src, dst.at[i], up_send.at[kind, i], up_recv.at[kind, i], above, col)

    def downward(kind, src, dst, i):
        return remote(src, dst.at[i], dn_send.at[kind, i], dn_recv.at[kind, i], below, col)

    next_shift = jnp.where(last, 1, 0)

    def home(i, src):
        return remote(src, out.at[twice0 + next_shift + i, 0], dn_send.at[2, i], dn_recv.at[2, i], below, col)

    def share(k, j):
        return remote(pan.at[k, col], pan.at[k, col], pan_send.at[k, j], pan_recv.at[k, j],
                      row, partner if j == n_x - 1 else peers[j])

    def came(k, j):
        origin = partner if j == n_x - 1 else lax.rem(x + n_x - 1 - j, n_x) * 2 + core
        return remote(pan.at[k, origin], pan.at[k, origin], pan_send.at[k, j], pan_recv.at[k, j], row, partner)

    def passed(k, j):
        origin = lax.rem(x + n_x - 1 - j, n_x) * 2 + core
        return remote(pan.at[k, origin], pan.at[k, origin], rel_send.at[k, j], rel_recv.at[k, j], row, partner)

    def passed_here(k, j):
        origin = lax.rem(x + n_x - 1 - j, n_x) * 2 + (1 - core)
        return remote(pan.at[k, origin], pan.at[k, origin], rel_send.at[k, j], rel_recv.at[k, j], row, partner)

    order = [0, n_x - 2] + list(range(1, n_x - 2))
    panels_in[0].wait()
    for j in order + [n_x - 1]:
        share(0, j).start()
    tiles_in.wait()
    for i in range(per):
        upward(0, xin.at[once0 + i + shift], u1, i).start()
    for k in range(1, 4):
        panels_in[k].wait()
        for j in order + [n_x - 1]:
            share(k, j).start()

    def pass_on(k):
        for j in order:
            came(k, j).wait_recv()
            passed(k, j).start()

    def settle(k):
        came(k, n_x - 1).wait_recv()
        for j in order:
            passed_here(k, j).wait_recv()

    def factor_chunks(*ks):
        at = [(k, i) for k in ks for i in range(per)]
        raw = [pan[k, :, i].reshape(2 * band, band) for k, i in at]
        for (k, i), (v_hi, v_lo, p_hi, p_lo) in zip(at, factor_panels(raw)):
            vv[k, i, 0] = v_hi
            vv[k, i, 1] = v_lo
            pp[k, i, 0] = p_hi
            pp[k, i, 1] = p_lo

    def apply(k, i, d, l, upper, lower):
        s_hi, s_lo = split(jnp.concatenate([upper, lower], axis=0))
        p_hi, p_lo = pp[k, i, 0], pp[k, i, 1]
        v_hi, v_lo = vv[k, i, 0], vv[k, i, 1]
        w_hi, w_lo = split(mm(p_hi, s_hi) + mm(p_hi, s_lo) + mm(p_lo, s_hi))
        change = mm(jnp.concatenate([v_hi, v_lo], axis=1), jnp.concatenate([w_hi, w_hi], axis=0)) + mm(v_hi, w_lo)
        active = flags[d, l] >= 0
        return (jnp.where(active, upper - change[:band], upper), jnp.where(active, lower - change[band:], lower))

    pass_on(0)
    settle(0)
    flags_copy.wait()
    factor_chunks(0)
    pass_on(1)

    def early(i, carry):
        l = twice0 + i
        upward(0, u1.at[i], u1, i).wait_recv()
        upper, lower = apply(0, i, 0, l, xin[l], u1[i])
        s1[i] = lower
        xb[i] = upper
        downward(0, s1.at[i], d1, i).start()

        @pl.when(jnp.logical_not(first))
        def _():
            upward(1, xb.at[i], us, i).start()

        @pl.when(first & (i > 0))
        def _():
            upward(1, xb.at[i], us, i - 1).start()

        return carry

    lax.fori_loop(0, per - 1, early, 0)
    pass_on(2)
    settle(1)
    settle(2)
    factor_chunks(1, 2)
    lax.fori_loop(per - 1, per, early, 0)

    @pl.when(first)
    def _():
        upward(1, xb.at[per - 1], us, per - 1).start()

    pass_on(3)

    def middle(i, carry):
        l = once0 + i

        @pl.when(first & (i == 0))
        def _():
            xq[...] = xin[once0]

        @pl.when(jnp.logical_not(first & (i == 0)))
        def _():
            j = i - shift
            downward(0, d1.at[j], d1, j).wait_recv()
            xq[...] = d1[j]

        upward(1, us.at[i], us, i).wait_recv()
        upper, lower = apply(1, i, 0, l, xq[...], us[i])
        upper, lower = apply(2, i, 1, l, upper, lower)
        ss[i] = lower
        xs[i] = upper
        downward(1, ss.at[i], ds, i).start()

        @pl.when(jnp.logical_not(first & (i == 0)))
        def _():
            upward(2, xs.at[i], u2, i - shift).start()

        return carry

    lax.fori_loop(0, 1, middle, 0)
    settle(3)
    factor_chunks(3)
    lax.fori_loop(1, per, middle, 0)

    @pl.when(first)
    def _():
        downward(0, d1.at[per - 1], d1, per - 1).wait_recv()
        xq[...] = jnp.where(flags[0, twice0] >= 0, xb[0], d1[per - 1])
        upward(2, xq, u2, per - 1).start()

    def late(i, carry):
        l = twice0 + i

        @pl.when(jnp.logical_not(first & (i == 0)))
        def _():
            j = i - shift
            downward(1, ds.at[j], ds, j).wait_recv()

            xc[...] = ds[j]

        @pl.when(first & (i == 0))
        def _():
            xc[...] = xq[...]
            downward(1, ds.at[per - 1], ds, per - 1).wait_recv()

        upward(2, u2.at[i], u2, i).wait_recv()
        upper, lower = apply(3, i, 1, l, xc[...], u2[i])
        s2[i] = lower
        xf[i] = upper
        @pl.when(last & (i == per - 1))
        def _():
            remote(s2.at[i], d2, dn_send.at[2, i], dn_recv.at[2, i], below, col).start()

        @pl.when(jnp.logical_not(last & (i == per - 1)))
        def _():
            home(i, s2.at[i]).start()


        @pl.when(jnp.logical_not(first & (i == 0)))
        def _():
            pltpu.make_async_copy(xf.at[i], out.at[l, 0], out_sem.at[i]).start()

        return carry

    lax.fori_loop(0, per, late, 0)

    def close(i, carry):
        @pl.when(jnp.logical_not(first & (i == 0)))
        def _():
            j = i - shift
            remote(s2.at[j], out.at[once0 + i, 0], dn_send.at[2, j], dn_recv.at[2, j], below, col).wait_recv()

        return carry

    lax.fori_loop(0, per, close, 0)

    @pl.when(first)
    def _():
        pltpu.make_async_copy(xs.at[0], out.at[once0, 0], out_sem.at[per]).start()
        remote(xq, d2, dn_send.at[2, per - 1], dn_recv.at[2, per - 1], below, col).wait_recv()
        xb[0] = jnp.where(flags[1, twice0] >= 0, xf[0], d2[...])
        pltpu.make_async_copy(xb.at[0], out.at[twice0, 0], out_sem.at[0]).start()
        pltpu.make_async_copy(xs.at[0], out.at[once0, 0], out_sem.at[per]).wait()

    def drain(i, carry):
        for kind in range(3):
            upward(kind, xb.at[i], u1, i).wait_send()
            downward(kind, xb.at[i], d1, i).wait_send()
        pltpu.make_async_copy(xf.at[i], out.at[twice0 + i, 0], out_sem.at[i]).wait()
        for j in range(n_x):
            share(i, j).wait_send()
        for j in range(n_x - 1):
            passed(i, j).wait_send()
        return carry

    lax.fori_loop(0, 4, drain, 0)


def local(n_row, n_x, eigvec, reflectors, sweep_group):
    tiles, _, band, width = eigvec.shape
    rows = reflectors.shape[3]
    per = tiles // 2
    tile = pltpu.VMEM((per, band, width), f32)
    dma = pltpu.SemaphoreType.DMA
    hbm = lambda array: pltpu.with_memory_space_constraint(array, pltpu.HBM)
    return pl.pallas_call(
        functools.partial(kernel, n_row, n_x),
        out_shape=jax.ShapeDtypeStruct(eigvec.shape, f32),
        in_specs=[pl.BlockSpec(memory_space=pltpu.HBM)] * 3,
        out_specs=pl.BlockSpec(memory_space=pl.ANY),
        scratch_shapes=[
            pltpu.SMEM(sweep_group.shape[:2], jnp.int32),
            pltpu.VMEM((tiles, band, width), f32),
            tile, tile, tile, pltpu.VMEM((band, width), f32), pltpu.VMEM((band, width), f32),
            tile, tile, tile, tile, tile, tile, tile, tile, pltpu.VMEM((band, width), f32),
            pltpu.VMEM((4, 2 * n_x, per, rows, band), f32),
            pltpu.VMEM((4, per, 2, 2 * band, band), bf16),
            pltpu.VMEM((4, per, 2, band, 2 * band), bf16),
            dma, dma, dma((4,)), dma((4, n_x)), dma((4, n_x)), dma((4, n_x - 1)), dma((4, n_x - 1)),
            dma((3, per)), dma((3, per)), dma((3, per)), dma((3, per)), dma((per + 1,)),
        ],
        compiler_params=pltpu.CompilerParams(
            collective_id=0, has_side_effects=True, vmem_limit_bytes=48 * 1024 * 1024),
    )(hbm(eigvec), hbm(reflectors), hbm(sweep_group.reshape(sweep_group.shape[:2])))


def solution(mesh):
    return jax.shard_map(
        functools.partial(local, mesh.shape["row"], mesh.shape["col"] // 2),
        mesh=mesh,
        in_specs=(
            P(None, "row", None, "col"),
            P(None, None, "row", "col", None),
            P(None, None, "row"),
        ),
        out_specs=P(None, "row", None, "col"),
        check_vma=False,
    )
```

```python
import functools

import jax
import jax.numpy as jnp
from jax import lax
from jax.experimental import pallas as pl
from jax.experimental.pallas import tpu as pltpu
from jax.sharding import PartitionSpec as P

MESH = pl.DeviceIdType.MESH
f32, bf16 = jnp.float32, jnp.bfloat16
TILES, FEWER = 8, 3


def split(a):
    hi = a.astype(bf16)
    return hi, (a - hi.astype(f32)).astype(bf16)


def mm(a, b):
    return jnp.dot(a, b, preferred_element_type=f32)


def square_dot(a, b):
    n = a.shape[-1]
    a_hi, a_lo = split(a)
    b_hi, b_lo = split(b)
    right = jnp.concatenate([b_hi, b_lo], axis=1)
    both = mm(jnp.concatenate([a_hi, a_lo], axis=1), jnp.concatenate([right, right], axis=0))
    return both[:, :n] + both[:, n:]


def factor_panels(panels):
    depth, band = panels[0].shape
    rows = lax.broadcasted_iota(jnp.int32, (depth, band), 0)
    cols = lax.broadcasted_iota(jnp.int32, (depth, band), 1)
    inside = (rows >= cols + 1) & (rows <= cols + band)
    leading = rows == cols + 1
    r = lax.broadcasted_iota(jnp.int32, (band, band), 0)
    c = lax.broadcasted_iota(jnp.int32, (band, band), 1)
    eye, above, beside = r == c, r < c, (r + 1 == c) & (lax.rem(c, 2) == 1)
    halves, turned, factors, inverses = [], [], [], []
    coupled = above & (r // 2 != c // 2) & (r // 4 == c // 4)
    for panel in panels:
        vectors = jnp.where(leading, 1.0, jnp.where(inside, panel, 0.0))
        v_hi, v_lo = split(vectors)
        t_hi, t_lo = split(vectors.T)
        both = mm(t_hi, jnp.concatenate([v_hi, v_lo], axis=1))
        gram = both[:, :band] + both[:, band:] + mm(t_lo, v_hi)
        on_diagonal = jnp.where(eye, gram, 0.0)
        along = 2.0 / jnp.sum(on_diagonal, axis=0, keepdims=True)
        down = 2.0 / jnp.sum(on_diagonal, axis=1, keepdims=True)
        pair = jnp.where(beside, gram * along * down, 0.0)
        pair_along = -jnp.sum(pair, axis=0, keepdims=True)
        pair_down = -jnp.sum(pair, axis=1, keepdims=True)
        inverse = jnp.where(eye, along, 0.0) - pair
        upper_part = jnp.where(coupled, gram, 0.0)
        middle = upper_part * along + pltpu.roll(upper_part, 1, 1) * pair_along
        inverse = inverse - (middle * down + pltpu.roll(middle, band - 1, 0) * pair_down)
        halves.append((v_hi, v_lo))
        turned.append((t_hi, t_lo))
        factors.append(gram)
        inverses.append(inverse)
    block = 4
    while block < band:
        step = 4 if 4 * block <= band else 2
        coupling = above & (r // block != c // block) & (r // (step * block) == c // (step * block))
        if step == 2:
            middles = [square_dot(jnp.where(coupling, f, 0.0), x) for f, x in zip(factors, inverses)]
            inverses = [x - square_dot(x, m) for x, m in zip(inverses, middles)]
        else:
            moves = [square_dot(x, jnp.where(coupling, f, 0.0)) for f, x in zip(factors, inverses)]
            squares = [square_dot(m, m) for m in moves]
            firsts = [x - square_dot(m, x) for m, x in zip(moves, inverses)]
            inverses = [y + square_dot(q, y) for q, y in zip(squares, firsts)]
        block *= step
    results = []
    for (v_hi, v_lo), (t_hi, t_lo), inverse in zip(halves, turned, inverses):
        i_hi, i_lo = split(inverse)
        solver = mm(jnp.concatenate([i_hi, i_lo], axis=1), jnp.concatenate([t_hi, t_hi], axis=0)) + mm(i_hi, t_lo)
        p_hi, p_lo = split(solver)
        results.append((v_hi, v_lo, p_hi, p_lo))
    return results


def kernel(n_row, n_x, fewer, *refs):
    odd = lax.rem(lax.axis_index("row"), 2) == 1

    @pl.when(odd)
    def _():
        body(n_row, n_x, (0, fewer), (fewer, TILES - fewer), 0, *refs)

    @pl.when(jnp.logical_not(odd))
    def _():
        body(n_row, n_x, (fewer, TILES - fewer), (0, fewer), 1, *refs)


def body(n_row, n_x, twice, once, held, eig, refl, flags_in, out,
         flags, xin, xb, xs, xf, xq, xc, u1, us, u2, s1, ss, s2, d1, ds, d2, pan, vv, pp,
         flag_sem, in_sem, pan_in, pan_send, pan_recv, fwd_send, fwd_recv, rel_send, rel_recv,
         up_send, up_recv, dn_send, dn_recv, out_sem):
    row = lax.axis_index("row")
    col = lax.axis_index("col")
    band = xin.shape[1]
    x, core = col // 2, lax.rem(col, 2)
    first = row == 0
    last = row == n_row - 1
    shift = jnp.where(first, 1, 0)
    next_shift = jnp.where(last, 1, 0)
    above = lax.rem(row + n_row - 1, n_row)
    below = lax.rem(row + 1, n_row)
    (twice0, n_twice), (once0, n_once) = twice, once
    partner = x * 2 + (1 - core)
    x_right, x_left, x_far = lax.rem(x + 1, n_x), lax.rem(x + n_x - 1, n_x), lax.rem(x + 2, n_x)
    right, left = x_right * 2 + core, x_left * 2 + core

    chunks = ((0, *twice), (0, *once), (1, *once), (1, *twice))

    def shares(k, c, half=None):
        d, l0, n = chunks[k]
        lo, hi = {None: (0, n), 0: (0, n // 2), 1: (n // 2, n)}[half]
        return pan.at[d, pl.ds(l0 + lo, hi - lo), c]

    tiles_in = pltpu.make_async_copy(eig.at[:, 0], xin, in_sem)
    tiles_in.start()
    panels_in = []
    for k, (d, l0, n) in enumerate(chunks):
        copy = pltpu.make_async_copy(refl.at[d, pl.ds(l0, n), 0], shares(k, col), pan_in.at[k])
        copy.start()
        panels_in.append(copy)
    flags_copy = pltpu.make_async_copy(flags_in, flags, flag_sem)
    flags_copy.start()

    barrier = pltpu.get_barrier_semaphore()
    for r_, c_ in ((above, col), (below, col), (row, right), (row, left), (row, partner)):
        pl.semaphore_signal(barrier, inc=1, device_id=(r_, c_), device_id_type=MESH)
    pl.semaphore_wait(barrier, 5)

    def remote(src, dst, ssem, rsem, r_, c_):
        return pltpu.make_async_remote_copy(src_ref=src, dst_ref=dst, send_sem=ssem, recv_sem=rsem,
                                            device_id=(r_, c_), device_id_type=MESH)

    def upward(kind, src, dst, i):
        return remote(src, dst.at[i], up_send.at[kind, i], up_recv.at[kind, i], above, col)

    def downward(kind, src, dst, i):
        return remote(src, dst.at[i], dn_send.at[kind, i], dn_recv.at[kind, i], below, col)

    def home(i, src):
        return remote(src, out.at[twice0 + next_shift + i, 0], dn_send.at[2, i], dn_recv.at[2, i], below, col)

    def given(k, j):
        c = shares(k, col)
        return remote(c, c, pan_send.at[k, j], pan_recv.at[k, j], row, (right, left, partner)[j])

    def taken(k, j):
        c = shares(k, (left, right, partner)[j])
        return remote(c, c, pan_send.at[k, j], pan_recv.at[k, j], row, partner)

    def onward(k, j):
        c = shares(k, (left, right)[j], j)
        return remote(c, c, fwd_send.at[k, j], fwd_recv.at[k, j], row, (right, left)[j])

    def onward_taken(k, j):
        c = shares(k, x_far * 2 + core, j)
        return remote(c, c, fwd_send.at[k, j], fwd_recv.at[k, j], row, partner)

    def across(k, j, c_):
        origin = (x_left, x_right, x_far, x_far)[j] * 2 + c_
        c = shares(k, origin, None if j < 2 else j - 2)
        return remote(c, c, rel_send.at[k, j], rel_recv.at[k, j], row, partner)

    def give(k):
        panels_in[k].wait()
        for j in range(3):
            given(k, j).start()

    def near(k):
        for j in range(2):
            taken(k, j).wait_recv()
            onward(k, j).start()
            across(k, j, core).start()

    def far(k):
        for j in range(2):
            onward_taken(k, j).wait_recv()
            across(k, 2 + j, core).start()

    def settle(k):
        taken(k, 2).wait_recv()
        for j in range(4):
            across(k, j, 1 - core).wait_recv()

    def factor_chunks(*ks):
        at = [(chunks[k][0], chunks[k][1] + i) for k in ks for i in range(chunks[k][2])]
        raw = [pan[d, l].reshape(2 * band, band) for d, l in at]
        for (d, l), (v_hi, v_lo, p_hi, p_lo) in zip(at, factor_panels(raw)):
            vv[d, l, 0] = v_hi
            vv[d, l, 1] = v_lo
            pp[d, l, 0] = p_hi
            pp[d, l, 1] = p_lo

    def apply(d, l, upper, lower):
        s_hi, s_lo = split(jnp.concatenate([upper, lower], axis=0))
        p_hi, p_lo = pp[d, l, 0], pp[d, l, 1]
        v_hi, v_lo = vv[d, l, 0], vv[d, l, 1]
        w_hi, w_lo = split(mm(p_hi, s_hi) + mm(p_hi, s_lo) + mm(p_lo, s_hi))
        change = mm(jnp.concatenate([v_hi, v_lo], axis=1), jnp.concatenate([w_hi, w_hi], axis=0)) + mm(v_hi, w_lo)
        active = flags[d, l] >= 0
        return (jnp.where(active, upper - change[:band], upper), jnp.where(active, lower - change[band:], lower))

    give(0)
    tiles_in.wait()
    for i in range(n_once):
        upward(0, xin.at[once0 + i + shift], u1, i).start()
    give(1)
    near(0)
    give(2)
    near(1)
    give(3)
    far(0)
    flags_copy.wait()
    settle(0)
    factor_chunks(0)
    far(1)
    near(2)

    def early(i, carry):
        upward(0, u1.at[i], u1, i).wait_recv()
        upper, lower = apply(0, twice0 + i, xin[twice0 + i], u1[i])
        s1[i] = lower
        xb[i] = upper
        downward(0, s1.at[i], d1, i).start()

        @pl.when(jnp.logical_not(first))
        def _():
            upward(1, xb.at[i], us, i).start()

        @pl.when(first & (i > 0))
        def _():
            upward(1, xb.at[i], us, i - 1).start()

        return carry

    lax.fori_loop(0, n_twice - held, early, 0)
    near(3)
    far(2)
    settle(1)
    settle(2)
    factor_chunks(1, 2)
    lax.fori_loop(n_twice - held, n_twice, early, 0)
    far(3)

    def middle(i, carry):
        l = once0 + i
        closed = last & (i == n_once - 1)

        @pl.when(first & (i == 0))
        def _():
            xq[...] = xin[once0]

        @pl.when(jnp.logical_not(first & (i == 0)))
        def _():
            j = i - shift
            downward(0, d1.at[j], d1, j).wait_recv()
            xq[...] = d1[j]

        @pl.when(jnp.logical_not(closed))
        def _():
            upward(1, us.at[i], us, i).wait_recv()
            xc[...] = us[i]

        upper, lower = apply(0, l, xq[...], xc[...])
        upper, lower = apply(1, l, upper, lower)
        ss[i] = lower
        xs[i] = upper

        @pl.when(jnp.logical_not(closed))
        def _():
            downward(1, ss.at[i], ds, i).start()

        @pl.when(jnp.logical_not(first & (i == 0)))
        def _():
            upward(2, xs.at[i], u2, i - shift).start()

        return carry

    lax.fori_loop(0, 1, middle, 0)
    settle(3)
    factor_chunks(3)
    lax.fori_loop(1, n_once, middle, 0)

    @pl.when(first)
    def _():
        downward(0, d1.at[n_once - 1], d1, n_once - 1).wait_recv()
        xq[...] = jnp.where(flags[0, twice0] >= 0, xb[0], d1[n_once - 1])
        upward(2, xq, u2, n_once - 1).start()

    def late(i, carry):
        @pl.when(jnp.logical_not(first & (i == 0)))
        def _():
            j = i - shift
            downward(1, ds.at[j], ds, j).wait_recv()
            xc[...] = ds[j]

        @pl.when(first & (i == 0))
        def _():
            xc[...] = xq[...]

        upward(2, u2.at[i], u2, i).wait_recv()
        upper, lower = apply(1, twice0 + i, xc[...], u2[i])
        s2[i] = lower
        xf[i] = upper

        @pl.when(last & (i == n_twice - 1))
        def _():
            remote(s2.at[i], d2, dn_send.at[2, i], dn_recv.at[2, i], below, col).start()

        @pl.when(jnp.logical_not(last & (i == n_twice - 1)))
        def _():
            home(i, s2.at[i]).start()

        @pl.when(jnp.logical_not(first & (i == 0)))
        def _():
            pltpu.make_async_copy(xf.at[i], out.at[twice0 + i, 0], out_sem.at[i]).start()

        return carry

    lax.fori_loop(0, n_twice, late, 0)

    def close(i, carry):
        @pl.when(jnp.logical_not(first & (i == 0)))
        def _():
            j = i - shift
            remote(s2.at[j], out.at[once0 + i, 0], dn_send.at[2, j], dn_recv.at[2, j], below, col).wait_recv()

        return carry

    lax.fori_loop(0, n_once, close, 0)

    @pl.when(first)
    def _():
        own = pltpu.make_async_copy(xs.at[0], out.at[once0, 0], out_sem.at[TILES])
        own.start()
        remote(xq, d2, dn_send.at[2, n_once - 1], dn_recv.at[2, n_once - 1], below, col).wait_recv()
        xb[0] = jnp.where(flags[1, twice0] >= 0, xf[0], d2[...])
        pltpu.make_async_copy(xb.at[0], out.at[twice0, 0], out_sem.at[0]).start()
        own.wait()

    def drain_twice(i, carry):
        downward(0, s1.at[i], d1, i).wait_send()
        home(i, s2.at[i]).wait_send()
        pltpu.make_async_copy(xf.at[i], out.at[twice0 + i, 0], out_sem.at[i]).wait()

        @pl.when(jnp.logical_not(first & (i == n_twice - 1)))
        def _():
            upward(1, xb.at[i], us, i).wait_send()

        return carry

    def drain_once(i, carry):
        upward(0, xs.at[i], u1, i).wait_send()
        upward(2, xs.at[i], u2, i).wait_send()

        @pl.when(jnp.logical_not(last & (i == n_once - 1)))
        def _():
            downward(1, ss.at[i], ds, i).wait_send()

        return carry

    lax.fori_loop(0, n_twice, drain_twice, 0)
    lax.fori_loop(0, n_once, drain_once, 0)
    for k in range(4):
        for j in range(3):
            given(k, j).wait_send()
        for j in range(2):
            onward(k, j).wait_send()
        for j in range(4):
            across(k, j, core).wait_send()


def local(n_row, n_x, eigvec, reflectors, sweep_group):
    tiles, _, band, width = eigvec.shape
    rows = reflectors.shape[3]
    diagonals = reflectors.shape[0]
    cap = max(FEWER, tiles - FEWER)
    one, many = pltpu.VMEM((band, width), f32), pltpu.VMEM((cap, band, width), f32)
    dma = pltpu.SemaphoreType.DMA
    hbm = lambda array: pltpu.with_memory_space_constraint(array, pltpu.HBM)
    flags = sweep_group.reshape(sweep_group.shape[:2])
    return pl.pallas_call(
        functools.partial(kernel, n_row, n_x, FEWER),
        out_shape=jax.ShapeDtypeStruct(eigvec.shape, f32),
        in_specs=[pl.BlockSpec(memory_space=pltpu.HBM)] * 3,
        out_specs=pl.BlockSpec(memory_space=pl.ANY),
        scratch_shapes=[
            pltpu.SMEM(flags.shape, jnp.int32),
            pltpu.VMEM((tiles, band, width), f32),
            many, many, many, one, one,
            many, many, many, many, many, many, many, many, one,
            pltpu.VMEM((diagonals, tiles, 2 * n_x, rows, band), f32),
            pltpu.VMEM((diagonals, tiles, 2, 2 * band, band), bf16),
            pltpu.VMEM((diagonals, tiles, 2, band, 2 * band), bf16),
            dma, dma, dma((4,)), dma((4, 3)), dma((4, 3)), dma((4, 2)), dma((4, 2)), dma((4, 4)), dma((4, 4)),
            dma((3, cap)), dma((3, cap)), dma((3, cap)), dma((3, cap)), dma((tiles + 1,)),
        ],
        compiler_params=pltpu.CompilerParams(
            collective_id=0, has_side_effects=True, vmem_limit_bytes=48 * 1024 * 1024),
    )(hbm(eigvec), hbm(reflectors), hbm(flags))


def solution(mesh):
    return jax.shard_map(
        functools.partial(local, mesh.shape["row"], mesh.shape["col"] // 2),
        mesh=mesh,
        in_specs=(
            P(None, "row", None, "col"),
            P(None, None, "row", "col", None),
            P(None, None, "row"),
        ),
        out_specs=P(None, "row", None, "col"),
        check_vma=False,
    )
```

```python
import functools

import jax
import jax.numpy as jnp
from jax import lax
from jax.experimental import pallas as pl
from jax.experimental.pallas import tpu as pltpu
from jax.sharding import PartitionSpec as P

MESH = pl.DeviceIdType.MESH
f32, bf16 = jnp.float32, jnp.bfloat16
TILES, FEWER = 8, 4


def split(a):
    hi = a.astype(bf16)
    return hi, (a - hi.astype(f32)).astype(bf16)


def mm(a, b):
    return jnp.dot(a, b, preferred_element_type=f32)


def square_dot(a, b):
    n = a.shape[-1]
    a_hi, a_lo = split(a)
    b_hi, b_lo = split(b)
    right = jnp.concatenate([b_hi, b_lo], axis=1)
    both = mm(jnp.concatenate([a_hi, a_lo], axis=1), jnp.concatenate([right, right], axis=0))
    return both[:, :n] + both[:, n:]


def factor_panels(panels):
    depth, band = panels[0].shape
    rows = lax.broadcasted_iota(jnp.int32, (depth, band), 0)
    cols = lax.broadcasted_iota(jnp.int32, (depth, band), 1)
    inside = (rows >= cols + 1) & (rows <= cols + band)
    leading = rows == cols + 1
    r = lax.broadcasted_iota(jnp.int32, (band, band), 0)
    c = lax.broadcasted_iota(jnp.int32, (band, band), 1)
    eye, above, beside = r == c, r < c, (r + 1 == c) & (lax.rem(c, 2) == 1)
    halves, turned, factors, inverses = [], [], [], []
    coupled = above & (r // 2 != c // 2) & (r // 4 == c // 4)
    for panel in panels:
        vectors = jnp.where(leading, 1.0, jnp.where(inside, panel, 0.0))
        v_hi, v_lo = split(vectors)
        t_hi, t_lo = split(vectors.T)
        both = mm(t_hi, jnp.concatenate([v_hi, v_lo], axis=1))
        gram = both[:, :band] + both[:, band:] + mm(t_lo, v_hi)
        on_diagonal = jnp.where(eye, gram, 0.0)
        along = 2.0 / jnp.sum(on_diagonal, axis=0, keepdims=True)
        down = 2.0 / jnp.sum(on_diagonal, axis=1, keepdims=True)
        pair = jnp.where(beside, gram * along * down, 0.0)
        pair_along = -jnp.sum(pair, axis=0, keepdims=True)
        pair_down = -jnp.sum(pair, axis=1, keepdims=True)
        inverse = jnp.where(eye, along, 0.0) - pair
        upper_part = jnp.where(coupled, gram, 0.0)
        middle = upper_part * along + pltpu.roll(upper_part, 1, 1) * pair_along
        inverse = inverse - (middle * down + pltpu.roll(middle, band - 1, 0) * pair_down)
        halves.append((v_hi, v_lo))
        turned.append((t_hi, t_lo))
        factors.append(gram)
        inverses.append(inverse)
    block = 4
    while block < band:
        step = 4 if 4 * block <= band else 2
        coupling = above & (r // block != c // block) & (r // (step * block) == c // (step * block))
        if step == 2:
            middles = [square_dot(jnp.where(coupling, f, 0.0), x) for f, x in zip(factors, inverses)]
            inverses = [x - square_dot(x, m) for x, m in zip(inverses, middles)]
        else:
            moves = [square_dot(x, jnp.where(coupling, f, 0.0)) for f, x in zip(factors, inverses)]
            squares = [square_dot(m, m) for m in moves]
            firsts = [x - square_dot(m, x) for m, x in zip(moves, inverses)]
            inverses = [y + square_dot(q, y) for q, y in zip(squares, firsts)]
        block *= step
    results = []
    for (v_hi, v_lo), (t_hi, t_lo), inverse in zip(halves, turned, inverses):
        i_hi, i_lo = split(inverse)
        solver = mm(jnp.concatenate([i_hi, i_lo], axis=1), jnp.concatenate([t_hi, t_hi], axis=0)) + mm(i_hi, t_lo)
        p_hi, p_lo = split(solver)
        results.append((v_hi, v_lo, p_hi, p_lo))
    return results


def kernel(n_row, n_x, fewer, *refs):
    odd = lax.rem(lax.axis_index("row"), 2) == 1

    @pl.when(odd)
    def _():
        body(n_row, n_x, (0, fewer), (fewer, TILES - fewer), *refs)

    @pl.when(jnp.logical_not(odd))
    def _():
        body(n_row, n_x, (fewer, TILES - fewer), (0, fewer), *refs)


def body(n_row, n_x, twice, once, eig, refl, flags_in, out,
         flags, xin, xb, xs, xf, xq, xc, u1, us, u2, s1, ss, s2, d1, ds, d2, pan, vv, pp,
         flag_sem, in_sem, pan_in, pan_send, pan_recv, rel_send, rel_recv,
         up_send, up_recv, dn_send, dn_recv, out_sem):
    row = lax.axis_index("row")
    col = lax.axis_index("col")
    band = xin.shape[1]
    x, core = col // 2, lax.rem(col, 2)
    first = row == 0
    last = row == n_row - 1
    shift = jnp.where(first, 1, 0)
    next_shift = jnp.where(last, 1, 0)
    above = lax.rem(row + n_row - 1, n_row)
    below = lax.rem(row + 1, n_row)
    (twice0, n_twice), (once0, n_once) = twice, once
    partner = x * 2 + (1 - core)
    x_right, x_left, x_far = lax.rem(x + 1, n_x), lax.rem(x + n_x - 1, n_x), lax.rem(x + 2, n_x)
    right, left, far = x_right * 2 + core, x_left * 2 + core, x_far * 2 + core

    lead = n_twice // 2
    chunks = ((0, twice0, lead), (0, twice0 + lead, n_twice - lead), (0, *once), (1, *once), (1, *twice))

    def shares(k, c):
        d, l0, n = chunks[k]
        return pan.at[d, pl.ds(l0, n), c]

    tiles_in = pltpu.make_async_copy(eig.at[:, 0], xin, in_sem)
    tiles_in.start()
    panels_in = []
    for k, (d, l0, n) in enumerate(chunks):
        copy = pltpu.make_async_copy(refl.at[d, pl.ds(l0, n), 0], shares(k, col), pan_in.at[k])
        copy.start()
        panels_in.append(copy)
    flags_copy = pltpu.make_async_copy(flags_in, flags, flag_sem)
    flags_copy.start()

    barrier = pltpu.get_barrier_semaphore()
    for r_, c_ in ((above, col), (below, col), (row, right), (row, left), (row, far), (row, partner)):
        pl.semaphore_signal(barrier, inc=1, device_id=(r_, c_), device_id_type=MESH)
    pl.semaphore_wait(barrier, 6)

    def remote(src, dst, ssem, rsem, r_, c_):
        return pltpu.make_async_remote_copy(src_ref=src, dst_ref=dst, send_sem=ssem, recv_sem=rsem,
                                            device_id=(r_, c_), device_id_type=MESH)

    def upward(kind, src, dst, i):
        return remote(src, dst.at[i], up_send.at[kind, i], up_recv.at[kind, i], above, col)

    def downward(kind, src, dst, i):
        return remote(src, dst.at[i], dn_send.at[kind, i], dn_recv.at[kind, i], below, col)

    def home(i, src):
        return remote(src, out.at[twice0 + next_shift + i, 0], dn_send.at[2, i], dn_recv.at[2, i], below, col)

    def given(k, j):
        c = shares(k, col)
        return remote(c, c, pan_send.at[k, j], pan_recv.at[k, j], row, (right, left, far, partner)[j])

    def taken(k, j):
        c = shares(k, (left, right, far, partner)[j])
        return remote(c, c, pan_send.at[k, j], pan_recv.at[k, j], row, partner)

    def across(k, j, c_):
        c = shares(k, (x_left, x_right, x_far)[j] * 2 + c_)
        return remote(c, c, rel_send.at[k, j], rel_recv.at[k, j], row, partner)

    def give(k):
        panels_in[k].wait()
        for j in (2, 0, 1, 3):
            given(k, j).start()

    def pass_on(k):
        for j in (0, 1, 2):
            taken(k, j).wait_recv()
            across(k, j, core).start()

    def settle(k):
        taken(k, 3).wait_recv()
        for j in range(3):
            across(k, j, 1 - core).wait_recv()

    def factor_chunks(*ks):
        at = [(chunks[k][0], chunks[k][1] + i) for k in ks for i in range(chunks[k][2])]
        raw = [pan[d, l].reshape(2 * band, band) for d, l in at]
        for (d, l), (v_hi, v_lo, p_hi, p_lo) in zip(at, factor_panels(raw)):
            vv[d, l, 0] = v_hi
            vv[d, l, 1] = v_lo
            pp[d, l, 0] = p_hi
            pp[d, l, 1] = p_lo

    def apply(d, l, upper, lower):
        s_hi, s_lo = split(jnp.concatenate([upper, lower], axis=0))
        p_hi, p_lo = pp[d, l, 0], pp[d, l, 1]
        v_hi, v_lo = vv[d, l, 0], vv[d, l, 1]
        w_hi, w_lo = split(mm(p_hi, s_hi) + mm(p_hi, s_lo) + mm(p_lo, s_hi))
        change = mm(jnp.concatenate([v_hi, v_lo], axis=1), jnp.concatenate([w_hi, w_hi], axis=0)) + mm(v_hi, w_lo)
        active = flags[d, l] >= 0
        return (jnp.where(active, upper - change[:band], upper), jnp.where(active, lower - change[band:], lower))

    give(0)
    tiles_in.wait()
    for i in range(n_once):
        upward(0, xin.at[once0 + i + shift], u1, i).start()
    for k in range(1, len(chunks)):
        give(k)
    pass_on(0)
    flags_copy.wait()
    settle(0)
    factor_chunks(0)
    pass_on(1)

    def early(i, carry):
        upward(0, u1.at[i], u1, i).wait_recv()
        upper, lower = apply(0, twice0 + i, xin[twice0 + i], u1[i])
        s1[i] = lower
        xb[i] = upper
        downward(0, s1.at[i], d1, i).start()

        @pl.when(jnp.logical_not(first))
        def _():
            upward(1, xb.at[i], us, i).start()

        @pl.when(first & (i > 0))
        def _():
            upward(1, xb.at[i], us, i - 1).start()

        return carry

    lax.fori_loop(0, lead, early, 0)
    pass_on(2)
    settle(1)
    factor_chunks(1)
    pass_on(3)
    lax.fori_loop(lead, n_twice - 1, early, 0)
    settle(2)
    settle(3)
    factor_chunks(2, 3)
    lax.fori_loop(n_twice - 1, n_twice, early, 0)
    pass_on(4)

    def middle(i, carry):
        l = once0 + i
        closed = last & (i == n_once - 1)

        @pl.when(first & (i == 0))
        def _():
            xq[...] = xin[once0]

        @pl.when(jnp.logical_not(first & (i == 0)))
        def _():
            j = i - shift
            downward(0, d1.at[j], d1, j).wait_recv()
            xq[...] = d1[j]

        @pl.when(jnp.logical_not(closed))
        def _():
            upward(1, us.at[i], us, i).wait_recv()
            xc[...] = us[i]

        upper, lower = apply(0, l, xq[...], xc[...])
        upper, lower = apply(1, l, upper, lower)
        ss[i] = lower
        xs[i] = upper

        @pl.when(jnp.logical_not(closed))
        def _():
            downward(1, ss.at[i], ds, i).start()

        @pl.when(jnp.logical_not(first & (i == 0)))
        def _():
            upward(2, xs.at[i], u2, i - shift).start()

        return carry

    lax.fori_loop(0, 2, middle, 0)
    settle(4)
    factor_chunks(4)
    lax.fori_loop(2, n_once, middle, 0)

    @pl.when(first)
    def _():
        downward(0, d1.at[n_once - 1], d1, n_once - 1).wait_recv()
        xq[...] = jnp.where(flags[0, twice0] >= 0, xb[0], d1[n_once - 1])
        upward(2, xq, u2, n_once - 1).start()

    def late(i, carry):
        @pl.when(jnp.logical_not(first & (i == 0)))
        def _():
            j = i - shift
            downward(1, ds.at[j], ds, j).wait_recv()
            xc[...] = ds[j]

        @pl.when(first & (i == 0))
        def _():
            xc[...] = xq[...]

        upward(2, u2.at[i], u2, i).wait_recv()
        upper, lower = apply(1, twice0 + i, xc[...], u2[i])
        s2[i] = lower
        xf[i] = upper

        @pl.when(last & (i == n_twice - 1))
        def _():
            remote(s2.at[i], d2, dn_send.at[2, i], dn_recv.at[2, i], below, col).start()

        @pl.when(jnp.logical_not(last & (i == n_twice - 1)))
        def _():
            home(i, s2.at[i]).start()

        @pl.when(jnp.logical_not(first & (i == 0)))
        def _():
            pltpu.make_async_copy(xf.at[i], out.at[twice0 + i, 0], out_sem.at[i]).start()

        return carry

    lax.fori_loop(0, n_twice, late, 0)

    def close(i, carry):
        @pl.when(jnp.logical_not(first & (i == 0)))
        def _():
            j = i - shift
            remote(s2.at[j], out.at[once0 + i, 0], dn_send.at[2, j], dn_recv.at[2, j], below, col).wait_recv()

        return carry

    lax.fori_loop(0, n_once, close, 0)

    @pl.when(first)
    def _():
        own = pltpu.make_async_copy(xs.at[0], out.at[once0, 0], out_sem.at[TILES])
        own.start()
        remote(xq, d2, dn_send.at[2, n_once - 1], dn_recv.at[2, n_once - 1], below, col).wait_recv()
        xb[0] = jnp.where(flags[1, twice0] >= 0, xf[0], d2[...])
        pltpu.make_async_copy(xb.at[0], out.at[twice0, 0], out_sem.at[0]).start()
        own.wait()

    def drain_twice(i, carry):
        downward(0, s1.at[i], d1, i).wait_send()
        home(i, s2.at[i]).wait_send()
        pltpu.make_async_copy(xf.at[i], out.at[twice0 + i, 0], out_sem.at[i]).wait()

        @pl.when(jnp.logical_not(first & (i == n_twice - 1)))
        def _():
            upward(1, xb.at[i], us, i).wait_send()

        return carry

    def drain_once(i, carry):
        upward(0, xs.at[i], u1, i).wait_send()
        upward(2, xs.at[i], u2, i).wait_send()

        @pl.when(jnp.logical_not(last & (i == n_once - 1)))
        def _():
            downward(1, ss.at[i], ds, i).wait_send()

        return carry

    lax.fori_loop(0, n_twice, drain_twice, 0)
    lax.fori_loop(0, n_once, drain_once, 0)
    for k in range(len(chunks)):
        for j in range(4):
            given(k, j).wait_send()
        for j in range(3):
            across(k, j, core).wait_send()


def local(n_row, n_x, eigvec, reflectors, sweep_group):
    tiles, _, band, width = eigvec.shape
    rows = reflectors.shape[3]
    diagonals = reflectors.shape[0]
    cap = max(FEWER, tiles - FEWER)
    one, many = pltpu.VMEM((band, width), f32), pltpu.VMEM((cap, band, width), f32)
    dma = pltpu.SemaphoreType.DMA
    hbm = lambda array: pltpu.with_memory_space_constraint(array, pltpu.HBM)
    flags = sweep_group.reshape(sweep_group.shape[:2])
    return pl.pallas_call(
        functools.partial(kernel, n_row, n_x, FEWER),
        out_shape=jax.ShapeDtypeStruct(eigvec.shape, f32),
        in_specs=[pl.BlockSpec(memory_space=pltpu.HBM)] * 3,
        out_specs=pl.BlockSpec(memory_space=pl.ANY),
        scratch_shapes=[
            pltpu.SMEM(flags.shape, jnp.int32),
            pltpu.VMEM((tiles, band, width), f32),
            many, many, many, one, one,
            many, many, many, many, many, many, many, many, one,
            pltpu.VMEM((diagonals, tiles, 2 * n_x, rows, band), f32),
            pltpu.VMEM((diagonals, tiles, 2, 2 * band, band), bf16),
            pltpu.VMEM((diagonals, tiles, 2, band, 2 * band), bf16),
            dma, dma, dma((5,)), dma((5, 4)), dma((5, 4)), dma((5, 3)), dma((5, 3)),
            dma((3, cap)), dma((3, cap)), dma((3, cap)), dma((3, cap)), dma((tiles + 1,)),
        ],
        compiler_params=pltpu.CompilerParams(
            collective_id=0, has_side_effects=True, vmem_limit_bytes=48 * 1024 * 1024),
    )(hbm(eigvec), hbm(reflectors), hbm(flags))


def solution(mesh):
    return jax.shard_map(
        functools.partial(local, mesh.shape["row"], mesh.shape["col"] // 2),
        mesh=mesh,
        in_specs=(
            P(None, "row", None, "col"),
            P(None, None, "row", "col", None),
            P(None, None, "row"),
        ),
        out_specs=P(None, "row", None, "col"),
        check_vma=False,
    )
```

```python
import functools

import jax
import jax.numpy as jnp
from jax import lax
from jax.experimental import pallas as pl
from jax.experimental.pallas import tpu as pltpu
from jax.sharding import PartitionSpec as P

MESH = pl.DeviceIdType.MESH
f32, bf16 = jnp.float32, jnp.bfloat16
TILES, FEWER = 8, 4


def split(a):
    hi = a.astype(bf16)
    return hi, (a - hi.astype(f32)).astype(bf16)


def mm(a, b):
    return jnp.dot(a, b, preferred_element_type=f32)


def square_dot(a, b):
    n = a.shape[-1]
    a_hi, a_lo = split(a)
    b_hi, b_lo = split(b)
    right = jnp.concatenate([b_hi, b_lo], axis=1)
    both = mm(jnp.concatenate([a_hi, a_lo], axis=1), jnp.concatenate([right, right], axis=0))
    return both[:, :n] + both[:, n:]


def factor_panels(panels):
    depth, band = panels[0].shape
    rows = lax.broadcasted_iota(jnp.int32, (depth, band), 0)
    cols = lax.broadcasted_iota(jnp.int32, (depth, band), 1)
    inside = (rows >= cols + 1) & (rows <= cols + band)
    leading = rows == cols + 1
    r = lax.broadcasted_iota(jnp.int32, (band, band), 0)
    c = lax.broadcasted_iota(jnp.int32, (band, band), 1)
    eye, above, beside = r == c, r < c, (r + 1 == c) & (lax.rem(c, 2) == 1)
    halves, turned, factors, inverses = [], [], [], []
    coupled = above & (r // 2 != c // 2) & (r // 4 == c // 4)
    for panel in panels:
        vectors = jnp.where(leading, 1.0, jnp.where(inside, panel, 0.0))
        v_hi, v_lo = split(vectors)
        t_hi, t_lo = split(vectors.T)
        both = mm(t_hi, jnp.concatenate([v_hi, v_lo], axis=1))
        gram = both[:, :band] + both[:, band:] + mm(t_lo, v_hi)
        on_diagonal = jnp.where(eye, gram, 0.0)
        along = 2.0 / jnp.sum(on_diagonal, axis=0, keepdims=True)
        down = 2.0 / jnp.sum(on_diagonal, axis=1, keepdims=True)
        pair = jnp.where(beside, gram * along * down, 0.0)
        pair_along = -jnp.sum(pair, axis=0, keepdims=True)
        pair_down = -jnp.sum(pair, axis=1, keepdims=True)
        inverse = jnp.where(eye, along, 0.0) - pair
        upper_part = jnp.where(coupled, gram, 0.0)
        middle = upper_part * along + pltpu.roll(upper_part, 1, 1) * pair_along
        inverse = inverse - (middle * down + pltpu.roll(middle, band - 1, 0) * pair_down)
        halves.append((v_hi, v_lo))
        turned.append((t_hi, t_lo))
        factors.append(gram)
        inverses.append(inverse)
    block = 4
    while block < band:
        step = 4 if 4 * block <= band else 2
        coupling = above & (r // block != c // block) & (r // (step * block) == c // (step * block))
        if step == 2:
            middles = [square_dot(jnp.where(coupling, f, 0.0), x) for f, x in zip(factors, inverses)]
            inverses = [x - square_dot(x, m) for x, m in zip(inverses, middles)]
        else:
            moves = [square_dot(x, jnp.where(coupling, f, 0.0)) for f, x in zip(factors, inverses)]
            squares = [square_dot(m, m) for m in moves]
            firsts = [x - square_dot(m, x) for m, x in zip(moves, inverses)]
            inverses = [y + square_dot(q, y) for q, y in zip(squares, firsts)]
        block *= step
    results = []
    for (v_hi, v_lo), (t_hi, t_lo), inverse in zip(halves, turned, inverses):
        i_hi, i_lo = split(inverse)
        solver = mm(jnp.concatenate([i_hi, i_lo], axis=1), jnp.concatenate([t_hi, t_hi], axis=0)) + mm(i_hi, t_lo)
        p_hi, p_lo = split(solver)
        results.append((v_hi, v_lo, p_hi, p_lo))
    return results


def kernel(n_row, n_x, fewer, *refs):
    odd = lax.rem(lax.axis_index("row"), 2) == 1

    @pl.when(odd)
    def _():
        body(n_row, n_x, (0, fewer), (fewer, TILES - fewer), *refs)

    @pl.when(jnp.logical_not(odd))
    def _():
        body(n_row, n_x, (fewer, TILES - fewer), (0, fewer), *refs)


def body(n_row, n_x, twice, once, eig, refl, flags_in, out,
         flags, flags_above, xin, xb, xs, xf, xq, xc, u1, us, u2, s1, ss, s2, d1, ds, d2, l1, pan, vv, pp, epan, ev, ep,
         flag_sem, twin_send, twin_recv, l1_send, l1_recv, in_sem, pan_in, pan_send, pan_recv, rel_send, rel_recv,
         up_send, up_recv, dn_send, dn_recv, out_sem):
    row = lax.axis_index("row")
    col = lax.axis_index("col")
    band = xin.shape[1]
    x, core = col // 2, lax.rem(col, 2)
    first = row == 0
    last = row == n_row - 1
    shift = jnp.where(first, 1, 0)
    next_shift = jnp.where(last, 1, 0)
    above = lax.rem(row + n_row - 1, n_row)
    below = lax.rem(row + 1, n_row)
    (twice0, n_twice), (once0, n_once) = twice, once
    partner = x * 2 + (1 - core)
    x_right, x_left, x_far = lax.rem(x + 1, n_x), lax.rem(x + n_x - 1, n_x), lax.rem(x + 2, n_x)
    right, left, far = x_right * 2 + core, x_left * 2 + core, x_far * 2 + core

    lead = n_twice // 2
    n_both, n_both_above = n_twice - 2, n_once - 2
    chunks = ((0, twice0, lead), (0, twice0 + lead, n_twice - lead), (0, *once), (1, *once), (1, *twice))

    def shares(k, c):
        if k == len(chunks):
            return epan.at[pl.ds(0, n_both_above), c]
        d, l0, n = chunks[k]
        return pan.at[d, pl.ds(l0, n), c]

    tiles_in = pltpu.make_async_copy(eig.at[:, 0], xin, in_sem)
    tiles_in.start()
    panels_in = []
    for k, (d, l0, n) in enumerate(chunks):
        copy = pltpu.make_async_copy(refl.at[d, pl.ds(l0, n), 0], shares(k, col), pan_in.at[k])
        copy.start()
        panels_in.append(copy)
    flags_copy = pltpu.make_async_copy(flags_in, flags, flag_sem)
    flags_copy.start()

    barrier = pltpu.get_barrier_semaphore()
    for r_, c_ in ((above, col), (below, col), (row, right), (row, left), (row, far), (row, partner)):
        pl.semaphore_signal(barrier, inc=1, device_id=(r_, c_), device_id_type=MESH)
    pl.semaphore_wait(barrier, 6)

    def remote(src, dst, ssem, rsem, r_, c_):
        return pltpu.make_async_remote_copy(src_ref=src, dst_ref=dst, send_sem=ssem, recv_sem=rsem,
                                            device_id=(r_, c_), device_id_type=MESH)

    def upward(kind, src, dst, i):
        return remote(src, dst.at[i], up_send.at[kind, i], up_recv.at[kind, i], above, col)

    def downward(kind, src, dst, i):
        return remote(src, dst.at[i], dn_send.at[kind, i], dn_recv.at[kind, i], below, col)

    def home(i, src):
        return remote(src, out.at[twice0 + next_shift + i, 0], dn_send.at[2, i], dn_recv.at[2, i], below, col)

    def given(k, j):
        c = shares(k, col)
        return remote(c, c, pan_send.at[k, j], pan_recv.at[k, j], row, (right, left, far, partner)[j])

    def taken(k, j):
        c = shares(k, (left, right, far, partner)[j])
        return remote(c, c, pan_send.at[k, j], pan_recv.at[k, j], row, partner)

    def across(k, j, c_):
        c = shares(k, (x_left, x_right, x_far)[j] * 2 + c_)
        return remote(c, c, rel_send.at[k, j], rel_recv.at[k, j], row, partner)

    def twin_panels(n):
        return remote(pan.at[0, pl.ds(twice0 + 1, n), col], epan.at[pl.ds(0, n), col], twin_send.at[0], twin_recv.at[0], below, col)

    twin_flags = remote(flags_in, flags_above, twin_send.at[1], twin_recv.at[1], below, col)

    def twin_tile(i):
        return remote(xin.at[twice0 + 1 + i], l1.at[i], l1_send.at[i], l1_recv.at[i], below, col)

    def give(k):
        if k == len(chunks):
            twin_panels(n_both_above).wait_recv()
        else:
            panels_in[k].wait()
        for j in (2, 0, 1, 3):
            given(k, j).start()

    def pass_on(k):
        for j in (0, 1, 2):
            taken(k, j).wait_recv()
            across(k, j, core).start()

    def settle(k):
        taken(k, 3).wait_recv()
        for j in range(3):
            across(k, j, 1 - core).wait_recv()

    def factor_chunks(*ks, with_above=False):
        at = [(chunks[k][0], chunks[k][1] + i) for k in ks for i in range(chunks[k][2])]
        raw = [pan[d, l].reshape(2 * band, band) for d, l in at]
        if with_above:
            raw += [epan[e].reshape(2 * band, band) for e in range(n_both_above)]
        results = factor_panels(raw)
        for (d, l), (v_hi, v_lo, p_hi, p_lo) in zip(at, results):
            vv[d, l, 0] = v_hi
            vv[d, l, 1] = v_lo
            pp[d, l, 0] = p_hi
            pp[d, l, 1] = p_lo

        if with_above:
            for e, (v_hi, v_lo, p_hi, p_lo) in enumerate(results[len(at):]):
                present = flags_above[0:1, once0 + 1 + e:once0 + 2 + e] >= 0
                ev[e, 0] = v_hi[band:]
                ev[e, 1] = v_lo[band:]
                ep[e, 0] = jnp.where(present, p_hi.astype(f32), 0.0).astype(bf16)
                ep[e, 1] = jnp.where(present, p_lo.astype(f32), 0.0).astype(bf16)

    def change_of(v_hi, v_lo, p_hi, p_lo, upper, lower):
        s_hi, s_lo = split(jnp.concatenate([upper, lower], axis=0))
        w_hi, w_lo = split(mm(p_hi, s_hi) + mm(p_hi, s_lo) + mm(p_lo, s_hi))
        return mm(jnp.concatenate([v_hi, v_lo], axis=1), jnp.concatenate([w_hi, w_hi], axis=0)) + mm(v_hi, w_lo)

    def apply(d, l, upper, lower):
        change = change_of(vv[d, l, 0], vv[d, l, 1], pp[d, l, 0], pp[d, l, 1], upper, lower)
        active = flags[d, l] >= 0
        return (jnp.where(active, upper - change[:band], upper), jnp.where(active, lower - change[band:], lower))

    give(0)
    tiles_in.wait()
    for i in range(n_once):
        upward(0, xin.at[once0 + i + shift], u1, i).start()
    give(1)
    twin_panels(n_both).start()
    twin_flags.start()
    for i in range(n_both):
        twin_tile(i).start()
    for k in range(2, len(chunks) + 1):
        give(k)
    pass_on(0)
    flags_copy.wait()
    settle(0)
    factor_chunks(0)
    pass_on(1)

    def early(i, carry):
        upward(0, u1.at[i], u1, i).wait_recv()
        upper, lower = apply(0, twice0 + i, xin[twice0 + i], u1[i])
        s1[i] = lower
        xb[i] = upper

        @pl.when((i == 0) | (i == n_twice - 1))
        def _():
            downward(0, s1.at[i], d1, i).start()

        @pl.when(jnp.logical_not(first))
        def _():
            upward(1, xb.at[i], us, i).start()

        @pl.when(first & (i > 0))
        def _():
            upward(1, xb.at[i], us, i - 1).start()

        return carry

    lax.fori_loop(0, lead, early, 0)
    pass_on(2)
    settle(1)
    factor_chunks(1)
    pass_on(3)
    lax.fori_loop(lead, n_twice - 1, early, 0)
    settle(2)
    settle(3)
    factor_chunks(2, 3)
    lax.fori_loop(n_twice - 1, n_twice, early, 0)
    pass_on(4)
    pass_on(5)

    def middle(i, carry):
        l = once0 + i
        closed = last & (i == n_once - 1)

        @pl.when(first & (i == 0))
        def _():
            xq[...] = xin[once0]

        j = i - shift

        @pl.when((j == 0) | (j == n_once - 1))
        def _():
            downward(0, d1.at[j], d1, j).wait_recv()
            xq[...] = d1[j]

        @pl.when((j > 0) & (j < n_once - 1))
        def _():
            e = j - 1
            twin_tile(e).wait_recv()
            own = xin[once0 + i]
            xq[...] = own - change_of(ev[e, 0], ev[e, 1], ep[e, 0], ep[e, 1], l1[e], own)

        @pl.when(jnp.logical_not(closed))
        def _():
            upward(1, us.at[i], us, i).wait_recv()
            xc[...] = us[i]

        upper, lower = apply(0, l, xq[...], xc[...])
        upper, lower = apply(1, l, upper, lower)
        ss[i] = lower
        xs[i] = upper

        @pl.when(jnp.logical_not(closed))
        def _():
            downward(1, ss.at[i], ds, i).start()

        @pl.when(jnp.logical_not(first & (i == 0)))
        def _():
            upward(2, xs.at[i], u2, i - shift).start()

        return carry

    lax.fori_loop(0, 1, middle, 0)
    settle(4)
    settle(5)
    twin_flags.wait_recv()
    factor_chunks(4, with_above=True)
    lax.fori_loop(1, n_once, middle, 0)

    @pl.when(first)
    def _():
        downward(0, d1.at[n_once - 1], d1, n_once - 1).wait_recv()
        xq[...] = jnp.where(flags[0, twice0] >= 0, xb[0], d1[n_once - 1])
        upward(2, xq, u2, n_once - 1).start()

    def late(i, carry):
        @pl.when(jnp.logical_not(first & (i == 0)))
        def _():
            j = i - shift
            downward(1, ds.at[j], ds, j).wait_recv()
            xc[...] = ds[j]

        @pl.when(first & (i == 0))
        def _():
            xc[...] = xq[...]

        upward(2, u2.at[i], u2, i).wait_recv()
        upper, lower = apply(1, twice0 + i, xc[...], u2[i])
        s2[i] = lower
        xf[i] = upper

        @pl.when(last & (i == n_twice - 1))
        def _():
            remote(s2.at[i], d2, dn_send.at[2, i], dn_recv.at[2, i], below, col).start()

        @pl.when(jnp.logical_not(last & (i == n_twice - 1)))
        def _():
            home(i, s2.at[i]).start()

        @pl.when(jnp.logical_not(first & (i == 0)))
        def _():
            pltpu.make_async_copy(xf.at[i], out.at[twice0 + i, 0], out_sem.at[i]).start()

        return carry

    lax.fori_loop(0, n_twice, late, 0)

    def close(i, carry):
        @pl.when(jnp.logical_not(first & (i == 0)))
        def _():
            j = i - shift
            remote(s2.at[j], out.at[once0 + i, 0], dn_send.at[2, j], dn_recv.at[2, j], below, col).wait_recv()

        return carry

    lax.fori_loop(0, n_once, close, 0)

    @pl.when(first)
    def _():
        own = pltpu.make_async_copy(xs.at[0], out.at[once0, 0], out_sem.at[TILES])
        own.start()
        remote(xq, d2, dn_send.at[2, n_once - 1], dn_recv.at[2, n_once - 1], below, col).wait_recv()
        xb[0] = jnp.where(flags[1, twice0] >= 0, xf[0], d2[...])
        pltpu.make_async_copy(xb.at[0], out.at[twice0, 0], out_sem.at[0]).start()
        own.wait()

    def drain_twice(i, carry):
        @pl.when((i == 0) | (i == n_twice - 1))
        def _():
            downward(0, s1.at[i], d1, i).wait_send()

        home(i, s2.at[i]).wait_send()
        pltpu.make_async_copy(xf.at[i], out.at[twice0 + i, 0], out_sem.at[i]).wait()

        @pl.when(jnp.logical_not(first & (i == n_twice - 1)))
        def _():
            upward(1, xb.at[i], us, i).wait_send()

        return carry

    def drain_once(i, carry):
        upward(0, xs.at[i], u1, i).wait_send()
        upward(2, xs.at[i], u2, i).wait_send()

        @pl.when(jnp.logical_not(last & (i == n_once - 1)))
        def _():
            downward(1, ss.at[i], ds, i).wait_send()

        return carry

    lax.fori_loop(0, n_twice, drain_twice, 0)
    lax.fori_loop(0, n_once, drain_once, 0)
    twin_panels(n_both).wait_send()
    twin_flags.wait_send()
    for i in range(n_both):
        twin_tile(i).wait_send()
    for k in range(len(chunks) + 1):
        for j in range(4):
            given(k, j).wait_send()
        for j in range(3):
            across(k, j, core).wait_send()


def local(n_row, n_x, eigvec, reflectors, sweep_group):
    tiles, _, band, width = eigvec.shape
    rows = reflectors.shape[3]
    diagonals = reflectors.shape[0]
    cap = max(FEWER, tiles - FEWER)
    one, many = pltpu.VMEM((band, width), f32), pltpu.VMEM((cap, band, width), f32)
    few = pltpu.VMEM((cap - 2, band, width), f32)
    dma = pltpu.SemaphoreType.DMA
    hbm = lambda array: pltpu.with_memory_space_constraint(array, pltpu.HBM)
    flags = sweep_group.reshape(sweep_group.shape[:2])
    return pl.pallas_call(
        functools.partial(kernel, n_row, n_x, FEWER),
        out_shape=jax.ShapeDtypeStruct(eigvec.shape, f32),
        in_specs=[pl.BlockSpec(memory_space=pltpu.HBM)] * 3,
        out_specs=pl.BlockSpec(memory_space=pl.ANY),
        scratch_shapes=[
            pltpu.SMEM(flags.shape, jnp.int32),
            pltpu.VMEM(flags.shape, jnp.int32),
            pltpu.VMEM((tiles, band, width), f32),
            many, many, many, one, one,
            many, many, many, many, many, many, many, many, one, few,
            pltpu.VMEM((diagonals, tiles, 2 * n_x, rows, band), f32),
            pltpu.VMEM((diagonals, tiles, 2, 2 * band, band), bf16),
            pltpu.VMEM((diagonals, tiles, 2, band, 2 * band), bf16),
            pltpu.VMEM((cap - 2, 2 * n_x, rows, band), f32),
            pltpu.VMEM((cap - 2, 2, band, band), bf16),
            pltpu.VMEM((cap - 2, 2, band, 2 * band), bf16),
            dma, dma((2,)), dma((2,)), dma((cap - 2,)), dma((cap - 2,)),
            dma, dma((5,)), dma((6, 4)), dma((6, 4)), dma((6, 3)), dma((6, 3)),
            dma((3, cap)), dma((3, cap)), dma((3, cap)), dma((3, cap)), dma((tiles + 1,)),
        ],
        compiler_params=pltpu.CompilerParams(
            collective_id=0, has_side_effects=True, vmem_limit_bytes=48 * 1024 * 1024),
    )(hbm(eigvec), hbm(reflectors), hbm(flags))


def solution(mesh):
    return jax.shard_map(
        functools.partial(local, mesh.shape["row"], mesh.shape["col"] // 2),
        mesh=mesh,
        in_specs=(
            P(None, "row", None, "col"),
            P(None, None, "row", "col", None),
            P(None, None, "row"),
        ),
        out_specs=P(None, "row", None, "col"),
        check_vma=False,
    )
```

```python
import functools

import jax
import jax.numpy as jnp
from jax import lax
from jax.experimental import pallas as pl
from jax.experimental.pallas import tpu as pltpu
from jax.sharding import PartitionSpec as P

MESH = pl.DeviceIdType.MESH
f32, bf16 = jnp.float32, jnp.bfloat16
TILES, FEWER, BOTH = 8, 4, 1


def split(a):
    hi = a.astype(bf16)
    return hi, (a - hi.astype(f32)).astype(bf16)


def mm(a, b):
    return jnp.dot(a, b, preferred_element_type=f32)


def square_dot(a, b):
    n = a.shape[-1]
    a_hi, a_lo = split(a)
    b_hi, b_lo = split(b)
    right = jnp.concatenate([b_hi, b_lo], axis=1)
    both = mm(jnp.concatenate([a_hi, a_lo], axis=1), jnp.concatenate([right, right], axis=0))
    return both[:, :n] + both[:, n:]


def factor_panels(panels):
    depth, band = panels[0].shape
    rows = lax.broadcasted_iota(jnp.int32, (depth, band), 0)
    cols = lax.broadcasted_iota(jnp.int32, (depth, band), 1)
    inside = (rows >= cols + 1) & (rows <= cols + band)
    leading = rows == cols + 1
    r = lax.broadcasted_iota(jnp.int32, (band, band), 0)
    c = lax.broadcasted_iota(jnp.int32, (band, band), 1)
    eye, above, beside = r == c, r < c, (r + 1 == c) & (lax.rem(c, 2) == 1)
    halves, turned, factors, inverses = [], [], [], []
    coupled = above & (r // 2 != c // 2) & (r // 4 == c // 4)
    for panel in panels:
        vectors = jnp.where(leading, 1.0, jnp.where(inside, panel, 0.0))
        v_hi, v_lo = split(vectors)
        t_hi, t_lo = split(vectors.T)
        both = mm(t_hi, jnp.concatenate([v_hi, v_lo], axis=1))
        gram = both[:, :band] + both[:, band:] + mm(t_lo, v_hi)
        on_diagonal = jnp.where(eye, gram, 0.0)
        along = 2.0 / jnp.sum(on_diagonal, axis=0, keepdims=True)
        down = 2.0 / jnp.sum(on_diagonal, axis=1, keepdims=True)
        pair = jnp.where(beside, gram * along * down, 0.0)
        pair_along = -jnp.sum(pair, axis=0, keepdims=True)
        pair_down = -jnp.sum(pair, axis=1, keepdims=True)
        inverse = jnp.where(eye, along, 0.0) - pair
        upper_part = jnp.where(coupled, gram, 0.0)
        middle = upper_part * along + pltpu.roll(upper_part, 1, 1) * pair_along
        inverse = inverse - (middle * down + pltpu.roll(middle, band - 1, 0) * pair_down)
        halves.append((v_hi, v_lo))
        turned.append((t_hi, t_lo))
        factors.append(gram)
        inverses.append(inverse)
    block = 4
    while block < band:
        step = 4 if 4 * block <= band else 2
        coupling = above & (r // block != c // block) & (r // (step * block) == c // (step * block))
        if step == 2:
            middles = [square_dot(jnp.where(coupling, f, 0.0), x) for f, x in zip(factors, inverses)]
            inverses = [x - square_dot(x, m) for x, m in zip(inverses, middles)]
        else:
            moves = [square_dot(x, jnp.where(coupling, f, 0.0)) for f, x in zip(factors, inverses)]
            squares = [square_dot(m, m) for m in moves]
            firsts = [x - square_dot(m, x) for m, x in zip(moves, inverses)]
            inverses = [y + square_dot(q, y) for q, y in zip(squares, firsts)]
        block *= step
    results = []
    for (v_hi, v_lo), (t_hi, t_lo), inverse in zip(halves, turned, inverses):
        i_hi, i_lo = split(inverse)
        solver = mm(jnp.concatenate([i_hi, i_lo], axis=1), jnp.concatenate([t_hi, t_hi], axis=0)) + mm(i_hi, t_lo)
        p_hi, p_lo = split(solver)
        results.append((v_hi, v_lo, p_hi, p_lo))
    return results


def kernel(n_row, n_x, fewer, *refs):
    odd = lax.rem(lax.axis_index("row"), 2) == 1

    @pl.when(odd)
    def _():
        body(n_row, n_x, (0, fewer), (fewer, TILES - fewer), *refs)

    @pl.when(jnp.logical_not(odd))
    def _():
        body(n_row, n_x, (fewer, TILES - fewer), (0, fewer), *refs)


def body(n_row, n_x, twice, once, eig, refl, flags_in, out,
         flags, flags_above, xin, xb, xs, xf, xq, xc, xz, u1, us, u2, s1, ss, s2, d1, ds, d2, l1, pan, vv, pp, epan, ev, ep,
         flag_sem, twin_send, twin_recv, l1_send, l1_recv, in_sem, pan_in, pan_send, pan_recv, rel_send, rel_recv,
         up_send, up_recv, dn_send, dn_recv, out_sem):
    row = lax.axis_index("row")
    col = lax.axis_index("col")
    band = xin.shape[1]
    x, core = col // 2, lax.rem(col, 2)
    first = row == 0
    last = row == n_row - 1
    shift = jnp.where(first, 1, 0)
    next_shift = jnp.where(last, 1, 0)
    above = lax.rem(row + n_row - 1, n_row)
    below = lax.rem(row + 1, n_row)
    (twice0, n_twice), (once0, n_once) = twice, once
    partner = x * 2 + (1 - core)
    x_right, x_left, x_far = lax.rem(x + 1, n_x), lax.rem(x + n_x - 1, n_x), lax.rem(x + 2, n_x)
    right, left, far = x_right * 2 + 1, x_left * 2 + 1, x_far * 2 + 1

    both, lead = epan.shape[0], n_twice // 2
    half = n_once // 2
    chunks = ((0, twice0 + lead, n_twice - lead),
              (0, once0 + half, n_once - half), (1, once0 + half, n_once - half),
              (0, twice0, lead),
              (0, once0, half), (1, once0, half),
              None,
              (1, *twice))
    order = range(n_twice - 1, -1, -1)

    def ordered(p):
        return n_twice - 1 - p


    def shares(k, c):
        if chunks[k] is None:
            return epan.at[:, c]
        d, l0, n = chunks[k]
        return pan.at[d, pl.ds(l0, n), c]

    tiles_in = pltpu.make_async_copy(eig.at[:, 0], xin, in_sem)
    tiles_in.start()
    panels_in = []
    for k, chunk in enumerate(chunks):
        if chunk is None:
            panels_in.append(None)
            continue
        d, l0, n = chunk
        copy = pltpu.make_async_copy(refl.at[d, pl.ds(l0, n), 0], shares(k, col), pan_in.at[k])
        copy.start()
        panels_in.append(copy)
    flags_copy = pltpu.make_async_copy(flags_in, flags, flag_sem)
    flags_copy.start()

    barrier = pltpu.get_barrier_semaphore()
    for r_, c_ in ((above, col), (below, col), (row, partner)):
        pl.semaphore_signal(barrier, inc=1, device_id=(r_, c_), device_id_type=MESH)

    @pl.when(core == 1)
    def _():
        for x_ in (x_right, x_left, x_far):
            for c_ in range(2):
                pl.semaphore_signal(barrier, inc=1, device_id=(row, x_ * 2 + c_), device_id_type=MESH)

    pl.semaphore_wait(barrier, 6)

    def remote(src, dst, ssem, rsem, r_, c_):
        return pltpu.make_async_remote_copy(src_ref=src, dst_ref=dst, send_sem=ssem, recv_sem=rsem,
                                            device_id=(r_, c_), device_id_type=MESH)

    def upward(kind, src, dst, i):
        return remote(src, dst.at[i], up_send.at[kind, i], up_recv.at[kind, i], above, col)

    def downward(kind, src, dst, i):
        return remote(src, dst.at[i], dn_send.at[kind, i], dn_recv.at[kind, i], below, col)

    def home(i, src):
        return remote(src, out.at[twice0 + next_shift + i, 0], dn_send.at[2, i], dn_recv.at[2, i], below, col)

    def given(k, j):
        c = shares(k, col)
        return remote(c, c, pan_send.at[k, j], pan_recv.at[k, 2 * j + core], row, (right, left, far)[j])

    def given_partner(k):
        c = shares(k, col)
        return remote(c, c, pan_send.at[k, 3], pan_recv.at[k, 6], row, partner)

    def taken(k, j, c_):
        c = shares(k, (x_left, x_right, x_far)[j] * 2 + c_)
        return remote(c, c, pan_send.at[k, j], pan_recv.at[k, 2 * j + c_], row, partner)

    def taken_partner(k):
        c = shares(k, partner)
        return remote(c, c, pan_send.at[k, 3], pan_recv.at[k, 6], row, partner)

    def across(k, j, c_):
        c = shares(k, (x_left, x_right, x_far)[j] * 2 + c_)
        return remote(c, c, rel_send.at[k, 2 * j + c_], rel_recv.at[k, 2 * j + c_], row, partner)

    arrivals = [(j, c_) for j in range(3) for c_ in (1, 0)]

    twin_panels = remote(pan.at[0, pl.ds(twice0, both), col], epan.at[:, col], twin_send.at[0], twin_recv.at[0], below, col)
    twin_flags = remote(flags_in, flags_above, twin_send.at[1], twin_recv.at[1], below, col)

    def twin_tile(e):
        return remote(xin.at[twice0 + e], l1.at[e], l1_send.at[e], l1_recv.at[e], below, col)

    def give(k):
        if chunks[k] is None:
            twin_panels.wait_recv()
        else:
            panels_in[k].wait()
        given_partner(k).start()
        for j in (2, 0, 1):
            given(k, j).start()

    def pass_on(k):
        @pl.when(core == 1)
        def _():
            for j, c_ in arrivals:
                taken(k, j, c_).wait_recv()
                across(k, j, c_).start()

    def settle(k):
        taken_partner(k).wait_recv()

        @pl.when(core == 0)
        def _():
            for j, c_ in arrivals:
                across(k, j, c_).wait_recv()

    def factor_chunks(*ks):
        with_above = any(chunks[k] is None for k in ks)
        at = [(chunks[k][0], chunks[k][1] + i) for k in ks if chunks[k] for i in range(chunks[k][2])]
        raw = [pan[d, l].reshape(2 * band, band) for d, l in at]
        if with_above:
            raw += [epan[e].reshape(2 * band, band) for e in range(both)]
        results = factor_panels(raw)
        for (d, l), (v_hi, v_lo, p_hi, p_lo) in zip(at, results):
            vv[d, l, 0] = v_hi
            vv[d, l, 1] = v_lo
            pp[d, l, 0] = p_hi
            pp[d, l, 1] = p_lo

        if with_above:
            for e, (v_hi, v_lo, p_hi, p_lo) in enumerate(results[len(at):]):
                present = flags_above[0:1, once0 + e:once0 + e + 1] >= 0
                ev[e, 0] = v_hi[band:]
                ev[e, 1] = v_lo[band:]
                ep[e, 0] = jnp.where(present, p_hi.astype(f32), 0.0).astype(bf16)
                ep[e, 1] = jnp.where(present, p_lo.astype(f32), 0.0).astype(bf16)

    def change_of(v_hi, v_lo, p_hi, p_lo, upper, lower):
        s_hi, s_lo = split(jnp.concatenate([upper, lower], axis=0))
        w_hi, w_lo = split(mm(p_hi, s_hi) + mm(p_hi, s_lo) + mm(p_lo, s_hi))
        return mm(jnp.concatenate([v_hi, v_lo], axis=1), jnp.concatenate([w_hi, w_hi], axis=0)) + mm(v_hi, w_lo)

    def apply(d, l, upper, lower):
        change = change_of(vv[d, l, 0], vv[d, l, 1], pp[d, l, 0], pp[d, l, 1], upper, lower)
        active = flags[d, l] >= 0
        return (jnp.where(active, upper - change[:band], upper), jnp.where(active, lower - change[band:], lower))

    give(0)
    tiles_in.wait()
    for i in order:
        upward(0, xin.at[once0 + i + shift], u1, i).start()
    for k in (1, 2, 3):
        give(k)
    twin_panels.start()
    twin_flags.start()
    for e in range(both):
        twin_tile(e).start()
    for k in (4, 5):
        give(k)
    pass_on(0)
    flags_copy.wait()
    settle(0)
    factor_chunks(0)
    give(6)
    give(7)
    pass_on(1)
    pass_on(2)

    def early(p, carry):
        i = ordered(p)
        upward(0, u1.at[i], u1, i).wait_recv()
        upper, lower = apply(0, twice0 + i, xin[twice0 + i], u1[i])
        xb[i] = upper

        @pl.when(i >= both)
        def _():
            s1[i] = lower
            downward(0, s1.at[i], d1, i).start()

        @pl.when(jnp.logical_not(first))
        def _():
            upward(1, xb.at[i], us, i).start()

        @pl.when(first & (i > 0))
        def _():
            upward(1, xb.at[i], us, i - 1).start()

        return carry

    lax.fori_loop(0, n_twice - lead, early, 0)
    pass_on(3)
    settle(1)
    settle(2)
    settle(3)
    factor_chunks(1, 2, 3)
    lax.fori_loop(n_twice - lead, n_twice, early, 0)
    pass_on(4)
    pass_on(5)
    pass_on(6)

    @pl.when(first)
    def _():
        downward(0, d1.at[n_once - 1], d1, n_once - 1).wait_recv()
        xz[...] = jnp.where(flags[0, twice0] >= 0, xb[0], d1[n_once - 1])
        upward(2, xz, u2, n_once - 1).start()

    def middle(p, carry):
        i = ordered(p)
        l = once0 + i
        closed = last & (i == n_once - 1)

        @pl.when(first & (i == 0))
        def _():
            xq[...] = xin[once0]

        j = i - shift

        @pl.when(j >= both)
        def _():
            downward(0, d1.at[j], d1, j).wait_recv()
            xq[...] = d1[j]

        @pl.when((j >= 0) & (j < both))
        def _():
            twin_tile(j).wait_recv()
            own = xin[once0 + i]
            xq[...] = own - change_of(ev[j, 0], ev[j, 1], ep[j, 0], ep[j, 1], l1[j], own)

        @pl.when(closed)
        def _():
            xc[...] = xin[once0]

        @pl.when(jnp.logical_not(closed))
        def _():
            upward(1, us.at[i], us, i).wait_recv()
            xc[...] = us[i]

        upper, lower = apply(0, l, xq[...], xc[...])
        upper, lower = apply(1, l, upper, lower)
        ss[i] = lower
        xs[i] = upper

        @pl.when(jnp.logical_not(closed))
        def _():
            downward(1, ss.at[i], ds, i).start()

        @pl.when(jnp.logical_not(first & (i == 0)))
        def _():
            upward(2, xs.at[i], u2, i - shift).start()

        return carry

    lax.fori_loop(0, n_once - half, middle, 0)

    settle(4)
    settle(5)
    settle(6)
    twin_flags.wait_recv()
    factor_chunks(4, 5, 6)
    pass_on(7)
    lax.fori_loop(n_once - half, n_once, middle, 0)
    settle(7)
    factor_chunks(7)

    def late(p, carry):
        i = ordered(p)

        @pl.when(jnp.logical_not(first & (i == 0)))
        def _():
            j = i - shift
            downward(1, ds.at[j], ds, j).wait_recv()
            xc[...] = ds[j]

        @pl.when(first & (i == 0))
        def _():
            xc[...] = xz[...]

        upward(2, u2.at[i], u2, i).wait_recv()
        upper, lower = apply(1, twice0 + i, xc[...], u2[i])
        s2[i] = lower
        xf[i] = upper

        @pl.when(last & (i == n_twice - 1))
        def _():
            remote(s2.at[i], d2, dn_send.at[2, i], dn_recv.at[2, i], below, col).start()

        @pl.when(jnp.logical_not(last & (i == n_twice - 1)))
        def _():
            home(i, s2.at[i]).start()

        @pl.when(jnp.logical_not(first & (i == 0)))
        def _():
            pltpu.make_async_copy(xf.at[i], out.at[twice0 + i, 0], out_sem.at[i]).start()

        return carry

    lax.fori_loop(0, n_twice, late, 0)

    def drain_twice(i, carry):
        @pl.when(i >= both)
        def _():
            downward(0, s1.at[i], d1, i).wait_send()

        @pl.when(i < both)
        def _():
            twin_tile(i).wait_send()

        @pl.when(jnp.logical_not(first & (i == n_twice - 1)))
        def _():
            upward(1, xb.at[i], us, i).wait_send()

        return carry

    def drain_once(i, carry):
        upward(0, xs.at[i], u1, i).wait_send()
        upward(2, xs.at[i], u2, i).wait_send()

        @pl.when(jnp.logical_not(last & (i == n_once - 1)))
        def _():
            downward(1, ss.at[i], ds, i).wait_send()

        return carry

    lax.fori_loop(0, n_twice, drain_twice, 0)
    lax.fori_loop(0, n_once, drain_once, 0)
    twin_panels.wait_send()
    twin_flags.wait_send()
    for k in range(len(chunks)):
        for j in range(3):
            given(k, j).wait_send()
        given_partner(k).wait_send()

        @pl.when(core == 1)
        def _():
            for j, c_ in arrivals:
                across(k, j, c_).wait_send()

    def close(i, carry):
        @pl.when(jnp.logical_not(first & (i == 0)))
        def _():
            j = i - shift
            remote(s2.at[j], out.at[once0 + i, 0], dn_send.at[2, j], dn_recv.at[2, j], below, col).wait_recv()

        return carry

    lax.fori_loop(0, n_once, close, 0)

    @pl.when(first)
    def _():
        own = pltpu.make_async_copy(xs.at[0], out.at[once0, 0], out_sem.at[TILES])
        own.start()
        remote(xz, d2, dn_send.at[2, n_once - 1], dn_recv.at[2, n_once - 1], below, col).wait_recv()
        xb[0] = jnp.where(flags[1, twice0] >= 0, xf[0], d2[...])
        pltpu.make_async_copy(xb.at[0], out.at[twice0, 0], out_sem.at[0]).start()
        own.wait()

    def finish(i, carry):
        home(i, s2.at[i]).wait_send()
        pltpu.make_async_copy(xf.at[i], out.at[twice0 + i, 0], out_sem.at[i]).wait()
        return carry

    lax.fori_loop(0, n_twice, finish, 0)


def local(n_row, n_x, eigvec, reflectors, sweep_group):
    tiles, _, band, width = eigvec.shape
    rows = reflectors.shape[3]
    diagonals = reflectors.shape[0]
    cap = max(FEWER, tiles - FEWER)
    one, many = pltpu.VMEM((band, width), f32), pltpu.VMEM((cap, band, width), f32)
    pair = BOTH
    dma = pltpu.SemaphoreType.DMA
    hbm = lambda array: pltpu.with_memory_space_constraint(array, pltpu.HBM)
    flags = sweep_group.reshape(sweep_group.shape[:2])
    return pl.pallas_call(
        functools.partial(kernel, n_row, n_x, FEWER),
        out_shape=jax.ShapeDtypeStruct(eigvec.shape, f32),
        in_specs=[pl.BlockSpec(memory_space=pltpu.HBM)] * 3,
        out_specs=pl.BlockSpec(memory_space=pl.ANY),
        scratch_shapes=[
            pltpu.SMEM(flags.shape, jnp.int32),
            pltpu.VMEM(flags.shape, jnp.int32),
            pltpu.VMEM((tiles, band, width), f32),
            many, many, many, one, one, one,
            many, many, many, many, many, many, many, many, one, pltpu.VMEM((pair, band, width), f32),
            pltpu.VMEM((diagonals, tiles, 2 * n_x, rows, band), f32),
            pltpu.VMEM((diagonals, tiles, 2, 2 * band, band), bf16),
            pltpu.VMEM((diagonals, tiles, 2, band, 2 * band), bf16),
            pltpu.VMEM((pair, 2 * n_x, rows, band), f32),
            pltpu.VMEM((pair, 2, band, band), bf16),
            pltpu.VMEM((pair, 2, band, 2 * band), bf16),
            dma, dma((2,)), dma((2,)), dma((pair,)), dma((pair,)),
            dma, dma((8,)), dma((8, 4)), dma((8, 7)), dma((8, 6)), dma((8, 6)),
            dma((3, cap)), dma((3, cap)), dma((3, cap)), dma((3, cap)), dma((tiles + 1,)),
        ],
        compiler_params=pltpu.CompilerParams(
            collective_id=0, has_side_effects=True, vmem_limit_bytes=48 * 1024 * 1024),
    )(hbm(eigvec), hbm(reflectors), hbm(flags))


def solution(mesh):
    return jax.shard_map(
        functools.partial(local, mesh.shape["row"], mesh.shape["col"] // 2),
        mesh=mesh,
        in_specs=(
            P(None, "row", None, "col"),
            P(None, None, "row", "col", None),
            P(None, None, "row"),
        ),
        out_specs=P(None, "row", None, "col"),
        check_vma=False,
    )
```

```python
import functools

import jax
import jax.numpy as jnp
from jax import lax
from jax.experimental import pallas as pl
from jax.experimental.pallas import tpu as pltpu
from jax.sharding import PartitionSpec as P

MESH = pl.DeviceIdType.MESH
f32, bf16 = jnp.float32, jnp.bfloat16
TILES, FEWER, BOTH = 8, 4, 1


def split(a):
    hi = a.astype(bf16)
    return hi, (a - hi.astype(f32)).astype(bf16)


def mm(a, b):
    return jnp.dot(a, b, preferred_element_type=f32)


def square_dot(a, b):
    n = a.shape[-1]
    a_hi, a_lo = split(a)
    b_hi, b_lo = split(b)
    right = jnp.concatenate([b_hi, b_lo], axis=1)
    both = mm(jnp.concatenate([a_hi, a_lo], axis=1), jnp.concatenate([right, right], axis=0))
    return both[:, :n] + both[:, n:]


def factor_panels(panels):
    depth, band = panels[0].shape
    rows = lax.broadcasted_iota(jnp.int32, (depth, band), 0)
    cols = lax.broadcasted_iota(jnp.int32, (depth, band), 1)
    inside = (rows >= cols + 1) & (rows <= cols + band)
    leading = rows == cols + 1
    r = lax.broadcasted_iota(jnp.int32, (band, band), 0)
    c = lax.broadcasted_iota(jnp.int32, (band, band), 1)
    eye, above, beside = r == c, r < c, (r + 1 == c) & (lax.rem(c, 2) == 1)
    halves, turned, factors, inverses = [], [], [], []
    coupled = above & (r // 2 != c // 2) & (r // 4 == c // 4)
    for panel in panels:
        vectors = jnp.where(leading, 1.0, jnp.where(inside, panel, 0.0))
        v_hi, v_lo = split(vectors)
        t_hi, t_lo = split(vectors.T)
        both = mm(t_hi, jnp.concatenate([v_hi, v_lo], axis=1))
        gram = both[:, :band] + both[:, band:] + mm(t_lo, v_hi)
        on_diagonal = jnp.where(eye, gram, 0.0)
        along = 2.0 / jnp.sum(on_diagonal, axis=0, keepdims=True)
        down = 2.0 / jnp.sum(on_diagonal, axis=1, keepdims=True)
        pair = jnp.where(beside, gram * along * down, 0.0)
        pair_along = -jnp.sum(pair, axis=0, keepdims=True)
        pair_down = -jnp.sum(pair, axis=1, keepdims=True)
        inverse = jnp.where(eye, along, 0.0) - pair
        upper_part = jnp.where(coupled, gram, 0.0)
        middle = upper_part * along + pltpu.roll(upper_part, 1, 1) * pair_along
        inverse = inverse - (middle * down + pltpu.roll(middle, band - 1, 0) * pair_down)
        halves.append((v_hi, v_lo))
        turned.append((t_hi, t_lo))
        factors.append(gram)
        inverses.append(inverse)
    block = 4
    while block < band:
        step = 4 if 4 * block <= band else 2
        coupling = above & (r // block != c // block) & (r // (step * block) == c // (step * block))
        if step == 2:
            middles = [square_dot(jnp.where(coupling, f, 0.0), x) for f, x in zip(factors, inverses)]
            inverses = [x - square_dot(x, m) for x, m in zip(inverses, middles)]
        else:
            moves = [square_dot(x, jnp.where(coupling, f, 0.0)) for f, x in zip(factors, inverses)]
            squares = [square_dot(m, m) for m in moves]
            firsts = [x - square_dot(m, x) for m, x in zip(moves, inverses)]
            inverses = [y + square_dot(q, y) for q, y in zip(squares, firsts)]
        block *= step
    results = []
    for (v_hi, v_lo), (t_hi, t_lo), inverse in zip(halves, turned, inverses):
        i_hi, i_lo = split(inverse)
        solver = mm(jnp.concatenate([i_hi, i_lo], axis=1), jnp.concatenate([t_hi, t_hi], axis=0)) + mm(i_hi, t_lo)
        p_hi, p_lo = split(solver)
        results.append((v_hi, v_lo, p_hi, p_lo))
    return results


def kernel(n_row, n_x, fewer, *refs):
    odd = lax.rem(lax.axis_index("row"), 2) == 1

    @pl.when(odd)
    def _():
        body(n_row, n_x, (0, fewer), (fewer, TILES - fewer), *refs)

    @pl.when(jnp.logical_not(odd))
    def _():
        body(n_row, n_x, (fewer, TILES - fewer), (0, fewer), *refs)


def body(n_row, n_x, twice, once, eig, refl, flags_in, out,
         flags, flags_above, xin, xb, xs, xf, xq, xc, xz, u1, us, u2, s1, ss, s2, d1, ds, d2, l1, pan, vv, pp, epan, ev, ep,
         flag_sem, twin_send, twin_recv, l1_send, l1_recv, in_sem, pan_in, pan_send, pan_recv, rel_send,
         up_send, up_recv, dn_send, dn_recv, out_sem):
    row = lax.axis_index("row")
    col = lax.axis_index("col")
    band = xin.shape[1]
    x, core = col // 2, lax.rem(col, 2)
    first = row == 0
    last = row == n_row - 1
    shift = jnp.where(first, 1, 0)
    next_shift = jnp.where(last, 1, 0)
    above = lax.rem(row + n_row - 1, n_row)
    below = lax.rem(row + 1, n_row)
    (twice0, n_twice), (once0, n_once) = twice, once
    partner = x * 2 + (1 - core)
    x_right, x_left, x_far = lax.rem(x + 1, n_x), lax.rem(x + n_x - 1, n_x), lax.rem(x + 2, n_x)
    right, left, far = x_right * 2 + 1, x_left * 2 + 1, x_far * 2 + 1

    both, lead = epan.shape[0], n_twice // 2
    half = n_once // 2
    chunks = ((0, twice0 + lead, n_twice - lead),
              (0, once0 + half, n_once - half), (1, once0 + half, n_once - half),
              (0, twice0, lead),
              (0, once0, half), (1, once0, half),
              None,
              (1, *twice))
    order = range(n_twice - 1, -1, -1)

    def ordered(p):
        return n_twice - 1 - p


    def shares(k, c):
        if chunks[k] is None:
            return epan.at[:, c]
        d, l0, n = chunks[k]
        return pan.at[d, pl.ds(l0, n), c]

    tiles_in = pltpu.make_async_copy(eig.at[:, 0], xin, in_sem)
    tiles_in.start()
    panels_in = pltpu.make_async_copy(refl.at[:, :, 0], pan.at[:, :, col], pan_in)
    panels_in.start()
    flags_copy = pltpu.make_async_copy(flags_in, flags, flag_sem)
    flags_copy.start()

    barrier = pltpu.get_barrier_semaphore()
    for r_, c_ in ((above, col), (below, col), (row, partner)):
        pl.semaphore_signal(barrier, inc=1, device_id=(r_, c_), device_id_type=MESH)

    @pl.when(core == 1)
    def _():
        for x_ in (x_right, x_left, x_far):
            for c_ in range(2):
                pl.semaphore_signal(barrier, inc=1, device_id=(row, x_ * 2 + c_), device_id_type=MESH)

    pl.semaphore_wait(barrier, 6)

    def remote(src, dst, ssem, rsem, r_, c_):
        return pltpu.make_async_remote_copy(src_ref=src, dst_ref=dst, send_sem=ssem, recv_sem=rsem,
                                            device_id=(r_, c_), device_id_type=MESH)

    def upward(kind, src, dst, i):
        return remote(src, dst.at[i], up_send.at[kind], up_recv.at[kind, i], above, col)

    def downward(kind, src, dst, i):
        return remote(src, dst.at[i], dn_send.at[kind], dn_recv.at[kind, i], below, col)

    def home(i, src):
        return remote(src, out.at[twice0 + next_shift + i, 0], dn_send.at[2], dn_recv.at[2, i], below, col)

    def given(k, j):
        c = shares(k, col)
        return remote(c, c, pan_send.at[k], pan_recv.at[k], row, (right, left, far, partner)[j])

    def across(k, j, c_):
        c = shares(k, (x_left, x_right, x_far)[j] * 2 + c_)
        return remote(c, c, rel_send.at[k], pan_recv.at[k], row, partner)

    def amount(k, n, send_sem):
        if chunks[k] is None:
            c = epan.at[:, pl.ds(0, n)]
        else:
            d, l0, m = chunks[k]
            c = pan.at[d, pl.ds(l0, m), pl.ds(0, n)]
        return remote(c, c, send_sem.at[k], pan_recv.at[k], row, partner)

    arrivals = [(j, c_) for j in range(3) for c_ in (1, 0)]

    twin_panels = remote(pan.at[0, pl.ds(twice0, both), col], epan.at[:, col], twin_send.at[0], twin_recv.at[0], below, col)
    twin_flags = remote(flags_in, flags_above, twin_send.at[1], twin_recv.at[1], below, col)

    def twin_tile(e):
        return remote(xin.at[twice0 + e], l1.at[e], l1_send.at[e], l1_recv.at[e], below, col)

    def give(k):
        if chunks[k] is None:
            twin_panels.wait_recv()
        for j in (3, 2, 0, 1):
            given(k, j).start()

    def pass_on(k):
        @pl.when(core == 1)
        def _():
            amount(k, 2 * n_x - 1, pan_send).wait_recv()
            for j, c_ in arrivals:
                across(k, j, c_).start()

    def settle(k):
        @pl.when(core == 0)
        def _():
            amount(k, 2 * n_x - 1, pan_send).wait_recv()

    def factor_chunks(*ks):
        with_above = any(chunks[k] is None for k in ks)
        at = [(chunks[k][0], chunks[k][1] + i) for k in ks if chunks[k] for i in range(chunks[k][2])]
        raw = [pan[d, l].reshape(2 * band, band) for d, l in at]
        if with_above:
            raw += [epan[e].reshape(2 * band, band) for e in range(both)]
        results = factor_panels(raw)
        for (d, l), (v_hi, v_lo, p_hi, p_lo) in zip(at, results):
            vv[d, l, 0] = v_hi
            vv[d, l, 1] = v_lo
            pp[d, l, 0] = p_hi
            pp[d, l, 1] = p_lo

        if with_above:
            for e, (v_hi, v_lo, p_hi, p_lo) in enumerate(results[len(at):]):
                present = flags_above[0:1, once0 + e:once0 + e + 1] >= 0
                ev[e, 0] = v_hi[band:]
                ev[e, 1] = v_lo[band:]
                ep[e, 0] = jnp.where(present, p_hi.astype(f32), 0.0).astype(bf16)
                ep[e, 1] = jnp.where(present, p_lo.astype(f32), 0.0).astype(bf16)

    def change_of(v_hi, v_lo, p_hi, p_lo, upper, lower):
        s_hi, s_lo = split(jnp.concatenate([upper, lower], axis=0))
        w_hi, w_lo = split(mm(p_hi, s_hi) + mm(p_hi, s_lo) + mm(p_lo, s_hi))
        return mm(jnp.concatenate([v_hi, v_lo], axis=1), jnp.concatenate([w_hi, w_hi], axis=0)) + mm(v_hi, w_lo)

    def apply(d, l, upper, lower):
        change = change_of(vv[d, l, 0], vv[d, l, 1], pp[d, l, 0], pp[d, l, 1], upper, lower)
        active = flags[d, l] >= 0
        return (jnp.where(active, upper - change[:band], upper), jnp.where(active, lower - change[band:], lower))

    panels_in.wait()
    give(0)
    tiles_in.wait()
    for i in order:
        upward(0, xin.at[once0 + i + shift], u1, i).start()
    for k in (1, 2, 3):
        give(k)
    twin_panels.start()
    twin_flags.start()
    for e in range(both):
        twin_tile(e).start()
    for k in (4, 5):
        give(k)
    pass_on(0)
    flags_copy.wait()
    settle(0)
    factor_chunks(0)
    give(6)
    give(7)
    pass_on(1)
    pass_on(2)

    def early(p, carry):
        i = ordered(p)
        upward(0, u1.at[i], u1, i).wait_recv()
        upper, lower = apply(0, twice0 + i, xin[twice0 + i], u1[i])
        xb[i] = upper

        @pl.when(i >= both)
        def _():
            s1[i] = lower
            downward(0, s1.at[i], d1, i).start()

        @pl.when(jnp.logical_not(first))
        def _():
            upward(1, xb.at[i], us, i).start()

        @pl.when(first & (i > 0))
        def _():
            upward(1, xb.at[i], us, i - 1).start()

        return carry

    lax.fori_loop(0, n_twice - lead, early, 0)
    pass_on(3)
    settle(1)
    settle(2)
    settle(3)
    factor_chunks(1, 2, 3)
    lax.fori_loop(n_twice - lead, n_twice, early, 0)
    pass_on(4)
    pass_on(5)
    pass_on(6)

    @pl.when(first)
    def _():
        downward(0, d1.at[n_once - 1], d1, n_once - 1).wait_recv()
        xz[...] = jnp.where(flags[0, twice0] >= 0, xb[0], d1[n_once - 1])
        upward(2, xz, u2, n_once - 1).start()

    def middle(p, carry):
        i = ordered(p)
        l = once0 + i
        closed = last & (i == n_once - 1)

        @pl.when(first & (i == 0))
        def _():
            xq[...] = xin[once0]

        j = i - shift

        @pl.when(j >= both)
        def _():
            downward(0, d1.at[j], d1, j).wait_recv()
            xq[...] = d1[j]

        @pl.when((j >= 0) & (j < both))
        def _():
            twin_tile(j).wait_recv()
            own = xin[once0 + i]
            xq[...] = own - change_of(ev[j, 0], ev[j, 1], ep[j, 0], ep[j, 1], l1[j], own)

        @pl.when(closed)
        def _():
            xc[...] = xin[once0]

        @pl.when(jnp.logical_not(closed))
        def _():
            upward(1, us.at[i], us, i).wait_recv()
            xc[...] = us[i]

        upper, lower = apply(0, l, xq[...], xc[...])
        upper, lower = apply(1, l, upper, lower)
        ss[i] = lower
        xs[i] = upper

        @pl.when(jnp.logical_not(closed))
        def _():
            downward(1, ss.at[i], ds, i).start()

        @pl.when(jnp.logical_not(first & (i == 0)))
        def _():
            upward(2, xs.at[i], u2, i - shift).start()

        return carry

    lax.fori_loop(0, n_once - half, middle, 0)

    settle(4)
    settle(5)
    settle(6)
    twin_flags.wait_recv()
    factor_chunks(4, 5, 6)
    pass_on(7)
    lax.fori_loop(n_once - half, n_once, middle, 0)
    settle(7)
    factor_chunks(7)

    def late(p, carry):
        i = ordered(p)

        @pl.when(jnp.logical_not(first & (i == 0)))
        def _():
            j = i - shift
            downward(1, ds.at[j], ds, j).wait_recv()
            xc[...] = ds[j]

        @pl.when(first & (i == 0))
        def _():
            xc[...] = xz[...]

        upward(2, u2.at[i], u2, i).wait_recv()
        upper, lower = apply(1, twice0 + i, xc[...], u2[i])
        s2[i] = lower
        xf[i] = upper

        @pl.when(last & (i == n_twice - 1))
        def _():
            remote(s2.at[i], d2, dn_send.at[2], dn_recv.at[2, i], below, col).start()

        @pl.when(jnp.logical_not(last & (i == n_twice - 1)))
        def _():
            home(i, s2.at[i]).start()

        @pl.when(jnp.logical_not(first & (i == 0)))
        def _():
            pltpu.make_async_copy(xf.at[i], out.at[twice0 + i, 0], out_sem.at[0]).start()

        return carry

    lax.fori_loop(0, n_twice, late, 0)

    def left_up(kind, n):
        remote(xs.at[pl.ds(0, n)], u1.at[pl.ds(0, n)], up_send.at[kind], up_recv.at[kind, 0], above, col).wait_send()

    def left_down(kind, n):
        remote(xs.at[pl.ds(0, n)], d1.at[pl.ds(0, n)], dn_send.at[kind], dn_recv.at[kind, 0], below, col).wait_send()

    left_up(0, n_once)
    left_up(2, n_once)
    left_down(0, n_twice - both)

    @pl.when(first)
    def _():
        left_up(1, n_twice - 1)

    @pl.when(jnp.logical_not(first))
    def _():
        left_up(1, n_twice)

    @pl.when(last)
    def _():
        left_down(1, n_once - 1)

    @pl.when(jnp.logical_not(last))
    def _():
        left_down(1, n_once)

    twin_panels.wait_send()
    twin_flags.wait_send()
    for e in range(both):
        twin_tile(e).wait_send()
    for k in range(len(chunks)):
        amount(k, n_x, pan_send).wait_send()

        @pl.when(core == 1)
        def _():
            amount(k, 2 * n_x - 2, rel_send).wait_send()

    def close(i, carry):
        @pl.when(jnp.logical_not(first & (i == 0)))
        def _():
            j = i - shift
            remote(s2.at[j], out.at[once0 + i, 0], dn_send.at[2], dn_recv.at[2, j], below, col).wait_recv()

        return carry

    lax.fori_loop(0, n_once, close, 0)

    @pl.when(first)
    def _():
        own = pltpu.make_async_copy(xs.at[0], out.at[once0, 0], out_sem.at[1])
        own.start()
        remote(xz, d2, dn_send.at[2], dn_recv.at[2, n_once - 1], below, col).wait_recv()
        xb[0] = jnp.where(flags[1, twice0] >= 0, xf[0], d2[...])
        pltpu.make_async_copy(xb.at[0], out.at[twice0, 0], out_sem.at[0]).start()
        own.wait()

    left_down(2, n_twice)
    pltpu.make_async_copy(xf, out.at[pl.ds(twice0, n_twice), 0], out_sem.at[0]).wait()


def local(n_row, n_x, eigvec, reflectors, sweep_group):
    tiles, _, band, width = eigvec.shape
    rows = reflectors.shape[3]
    diagonals = reflectors.shape[0]
    cap = max(FEWER, tiles - FEWER)
    one, many = pltpu.VMEM((band, width), f32), pltpu.VMEM((cap, band, width), f32)
    pair = BOTH
    dma = pltpu.SemaphoreType.DMA
    hbm = lambda array: pltpu.with_memory_space_constraint(array, pltpu.HBM)
    flags = sweep_group.reshape(sweep_group.shape[:2])
    return pl.pallas_call(
        functools.partial(kernel, n_row, n_x, FEWER),
        out_shape=jax.ShapeDtypeStruct(eigvec.shape, f32),
        in_specs=[pl.BlockSpec(memory_space=pltpu.HBM)] * 3,
        out_specs=pl.BlockSpec(memory_space=pl.ANY),
        scratch_shapes=[
            pltpu.SMEM(flags.shape, jnp.int32),
            pltpu.VMEM(flags.shape, jnp.int32),
            pltpu.VMEM((tiles, band, width), f32),
            many, many, many, one, one, one,
            many, many, many, many, many, many, many, many, one, pltpu.VMEM((pair, band, width), f32),
            pltpu.VMEM((diagonals, tiles, 2 * n_x, rows, band), f32),
            pltpu.VMEM((diagonals, tiles, 2, 2 * band, band), bf16),
            pltpu.VMEM((diagonals, tiles, 2, band, 2 * band), bf16),
            pltpu.VMEM((pair, 2 * n_x, rows, band), f32),
            pltpu.VMEM((pair, 2, band, band), bf16),
            pltpu.VMEM((pair, 2, band, 2 * band), bf16),
            dma, dma((2,)), dma((2,)), dma((pair,)), dma((pair,)),
            dma, dma, dma((8,)), dma((8,)), dma((8,)),
            dma((3,)), dma((3, cap)), dma((3,)), dma((3, cap)), dma((2,)),
        ],
        compiler_params=pltpu.CompilerParams(
            collective_id=0, has_side_effects=True, vmem_limit_bytes=48 * 1024 * 1024),
    )(hbm(eigvec), hbm(reflectors), hbm(flags))


def solution(mesh):
    return jax.shard_map(
        functools.partial(local, mesh.shape["row"], mesh.shape["col"] // 2),
        mesh=mesh,
        in_specs=(
            P(None, "row", None, "col"),
            P(None, None, "row", "col", None),
            P(None, None, "row"),
        ),
        out_specs=P(None, "row", None, "col"),
        check_vma=False,
    )
```

```python
import functools

import jax
import jax.numpy as jnp
from jax import lax
from jax.experimental import pallas as pl
from jax.experimental.pallas import tpu as pltpu
from jax.sharding import PartitionSpec as P

MESH = pl.DeviceIdType.MESH
f32, bf16 = jnp.float32, jnp.bfloat16
TILES, FEWER, BOTH = 8, 4, 1


def split(a):
    hi = a.astype(bf16)
    return hi, (a - hi.astype(f32)).astype(bf16)


def mm(a, b):
    return jnp.dot(a, b, preferred_element_type=f32)


def square_dot(a, b):
    n = a.shape[-1]
    a_hi, a_lo = split(a)
    b_hi, b_lo = split(b)
    right = jnp.concatenate([b_hi, b_lo], axis=1)
    both = mm(jnp.concatenate([a_hi, a_lo], axis=1), jnp.concatenate([right, right], axis=0))
    return both[:, :n] + both[:, n:]


def factor_panels(panels):
    depth, band = panels[0].shape
    rows = lax.broadcasted_iota(jnp.int32, (depth, band), 0)
    cols = lax.broadcasted_iota(jnp.int32, (depth, band), 1)
    inside = (rows >= cols + 1) & (rows <= cols + band)
    leading = rows == cols + 1
    r = lax.broadcasted_iota(jnp.int32, (band, band), 0)
    c = lax.broadcasted_iota(jnp.int32, (band, band), 1)
    eye, above, beside = r == c, r < c, (r + 1 == c) & (lax.rem(c, 2) == 1)
    halves, turned, factors, inverses = [], [], [], []
    coupled = above & (r // 2 != c // 2) & (r // 4 == c // 4)
    for panel in panels:
        vectors = jnp.where(leading, 1.0, jnp.where(inside, panel, 0.0))
        v_hi, v_lo = split(vectors)
        t_hi, t_lo = split(vectors.T)
        both = mm(t_hi, jnp.concatenate([v_hi, v_lo], axis=1))
        gram = both[:, :band] + both[:, band:] + mm(t_lo, v_hi)
        on_diagonal = jnp.where(eye, gram, 0.0)
        along = 2.0 / jnp.sum(on_diagonal, axis=0, keepdims=True)
        down = 2.0 / jnp.sum(on_diagonal, axis=1, keepdims=True)
        pair = jnp.where(beside, gram * along * down, 0.0)
        pair_along = -jnp.sum(pair, axis=0, keepdims=True)
        pair_down = -jnp.sum(pair, axis=1, keepdims=True)
        inverse = jnp.where(eye, along, 0.0) - pair
        upper_part = jnp.where(coupled, gram, 0.0)
        middle = upper_part * along + pltpu.roll(upper_part, 1, 1) * pair_along
        inverse = inverse - (middle * down + pltpu.roll(middle, band - 1, 0) * pair_down)
        halves.append((v_hi, v_lo))
        turned.append((t_hi, t_lo))
        factors.append(gram)
        inverses.append(inverse)
    block = 4
    while block < band:
        step = 4 if 4 * block <= band else 2
        coupling = above & (r // block != c // block) & (r // (step * block) == c // (step * block))
        if step == 2:
            middles = [square_dot(jnp.where(coupling, f, 0.0), x) for f, x in zip(factors, inverses)]
            inverses = [x - square_dot(x, m) for x, m in zip(inverses, middles)]
        else:
            moves = [square_dot(x, jnp.where(coupling, f, 0.0)) for f, x in zip(factors, inverses)]
            squares = [square_dot(m, m) for m in moves]
            firsts = [x - square_dot(m, x) for m, x in zip(moves, inverses)]
            inverses = [y + square_dot(q, y) for q, y in zip(squares, firsts)]
        block *= step
    results = []
    for (v_hi, v_lo), (t_hi, t_lo), inverse in zip(halves, turned, inverses):
        i_hi, i_lo = split(inverse)
        solver = mm(jnp.concatenate([i_hi, i_lo], axis=1), jnp.concatenate([t_hi, t_hi], axis=0)) + mm(i_hi, t_lo)
        p_hi, p_lo = split(solver)
        results.append((v_hi, v_lo, p_hi, p_lo))
    return results


def kernel(n_row, n_x, fewer, *refs):
    odd = lax.rem(lax.axis_index("row"), 2) == 1

    @pl.when(odd)
    def _():
        body(n_row, n_x, (0, fewer), (fewer, TILES - fewer), *refs)

    @pl.when(jnp.logical_not(odd))
    def _():
        body(n_row, n_x, (fewer, TILES - fewer), (0, fewer), *refs)


def body(n_row, n_x, twice, once, eig, refl, flags_in, out,
         flags, flags_above, xin, xb, xs, xf, xq, xc, xz, u1, us, u2, s1, ss, s2, d1, ds, d2, l1, pan, vv, pp, epan, ev, ep,
         flag_sem, twin_send, twin_recv, l1_send, l1_recv, in_sem, pan_in, pan_send, pan_recv, rel_send,
         up_send, up_recv, dn_send, dn_recv, out_sem):
    row = lax.axis_index("row")
    col = lax.axis_index("col")
    band = xin.shape[1]
    x, core = col // 2, lax.rem(col, 2)
    first = row == 0
    last = row == n_row - 1
    shift = jnp.where(first, 1, 0)
    next_shift = jnp.where(last, 1, 0)
    above = lax.rem(row + n_row - 1, n_row)
    below = lax.rem(row + 1, n_row)
    (twice0, n_twice), (once0, n_once) = twice, once
    partner = x * 2 + (1 - core)
    x_right, x_left, x_far = lax.rem(x + 1, n_x), lax.rem(x + n_x - 1, n_x), lax.rem(x + 2, n_x)
    right, left, far = x_right * 2 + 1, x_left * 2 + 1, x_far * 2 + 1

    both, lead = epan.shape[0], n_twice // 2
    half = n_once // 2
    chunks = ((0, twice0 + lead, n_twice - lead),
              (0, once0 + half, n_once - half), (1, once0 + half, n_once - half),
              (0, twice0, lead),
              (0, once0, half), (1, once0, half),
              None,
              (1, *twice))
    def ordered(p, n, swapped):
        return jnp.where(swapped & (p < 2), n - 2 + p, n - 1 - p)

    def shares(k, c):
        if chunks[k] is None:
            return epan.at[:, c]
        d, l0, n = chunks[k]
        return pan.at[d, pl.ds(l0, n), c]

    tiles_in = pltpu.make_async_copy(eig.at[:, 0], xin, in_sem)
    tiles_in.start()
    panels_in = pltpu.make_async_copy(refl.at[:, :, 0], pan.at[:, :, col], pan_in)
    panels_in.start()
    flags_copy = pltpu.make_async_copy(flags_in, flags, flag_sem)
    flags_copy.start()

    barrier = pltpu.get_barrier_semaphore()
    for r_, c_ in ((above, col), (below, col), (row, partner)):
        pl.semaphore_signal(barrier, inc=1, device_id=(r_, c_), device_id_type=MESH)

    @pl.when(core == 1)
    def _():
        for x_ in (x_right, x_left, x_far):
            for c_ in range(2):
                pl.semaphore_signal(barrier, inc=1, device_id=(row, x_ * 2 + c_), device_id_type=MESH)

    pl.semaphore_wait(barrier, 6)

    def remote(src, dst, ssem, rsem, r_, c_):
        return pltpu.make_async_remote_copy(src_ref=src, dst_ref=dst, send_sem=ssem, recv_sem=rsem,
                                            device_id=(r_, c_), device_id_type=MESH)

    def upward(kind, src, dst, i):
        return remote(src, dst.at[i], up_send.at[kind], up_recv.at[kind, i], above, col)

    def downward(kind, src, dst, i):
        return remote(src, dst.at[i], dn_send.at[kind], dn_recv.at[kind, i], below, col)

    def home(i, src):
        return remote(src, out.at[twice0 + next_shift + i, 0], dn_send.at[2], dn_recv.at[2, i], below, col)

    def given(k, j):
        c = shares(k, col)
        return remote(c, c, pan_send.at[1 if chunks[k] is None else 0], pan_recv.at[k], row, (right, left, far, partner)[j])

    def across(k, j, c_):
        c = shares(k, (x_left, x_right, x_far)[j] * 2 + c_)
        return remote(c, c, rel_send.at[1 if chunks[k] is None else 0], pan_recv.at[k], row, partner)

    def arrived(k):
        n = 2 * n_x - 1
        if chunks[k] is None:
            c = epan.at[:, pl.ds(0, n)]
        else:
            d, l0, m = chunks[k]
            c = pan.at[d, pl.ds(l0, m), pl.ds(0, n)]
        return remote(c, c, pan_send.at[0], pan_recv.at[k], row, partner)

    def departed(n, send_sem):
        own, other = pan.at[:, :, pl.ds(0, n)], epan.at[:, pl.ds(0, n)]
        remote(own, own, send_sem.at[0], pan_recv.at[0], row, partner).wait_send()
        remote(other, other, send_sem.at[1], pan_recv.at[0], row, partner).wait_send()

    arrivals = [(j, c_) for j in range(3) for c_ in (1, 0)]

    twin_panels = remote(pan.at[0, pl.ds(twice0, both), col], epan.at[:, col], twin_send.at[0], twin_recv.at[0], below, col)
    twin_flags = remote(flags_in, flags_above, twin_send.at[1], twin_recv.at[1], below, col)

    def twin_tile(e):
        return remote(xin.at[twice0 + e], l1.at[e], l1_send.at[e], l1_recv.at[e], below, col)

    def give(k):
        if chunks[k] is None:
            twin_panels.wait_recv()
        for j in (3, 2, 0, 1):
            given(k, j).start()

    def pass_on(k):
        @pl.when(core == 1)
        def _():
            arrived(k).wait_recv()
            for j, c_ in arrivals:
                across(k, j, c_).start()

    def settle(k):
        @pl.when(core == 0)
        def _():
            arrived(k).wait_recv()

    def factor_chunks(*ks):
        with_above = any(chunks[k] is None for k in ks)
        at = [(chunks[k][0], chunks[k][1] + i) for k in ks if chunks[k] for i in range(chunks[k][2])]
        raw = [pan[d, l].reshape(2 * band, band) for d, l in at]
        if with_above:
            raw += [epan[e].reshape(2 * band, band) for e in range(both)]
        results = factor_panels(raw)
        for (d, l), (v_hi, v_lo, p_hi, p_lo) in zip(at, results):
            vv[d, l, 0] = v_hi
            vv[d, l, 1] = v_lo
            pp[d, l, 0] = p_hi
            pp[d, l, 1] = p_lo

        if with_above:
            for e, (v_hi, v_lo, p_hi, p_lo) in enumerate(results[len(at):]):
                present = flags_above[0:1, once0 + e:once0 + e + 1] >= 0
                ev[e, 0] = v_hi[band:]
                ev[e, 1] = v_lo[band:]
                ep[e, 0] = jnp.where(present, p_hi.astype(f32), 0.0).astype(bf16)
                ep[e, 1] = jnp.where(present, p_lo.astype(f32), 0.0).astype(bf16)

    def change_of(v_hi, v_lo, p_hi, p_lo, upper, lower):
        s_hi, s_lo = split(jnp.concatenate([upper, lower], axis=0))
        w_hi, w_lo = split(mm(p_hi, s_hi) + mm(p_hi, s_lo) + mm(p_lo, s_hi))
        return mm(jnp.concatenate([v_hi, v_lo], axis=1), jnp.concatenate([w_hi, w_hi], axis=0)) + mm(v_hi, w_lo)

    def apply(d, l, upper, lower):
        change = change_of(vv[d, l, 0], vv[d, l, 1], pp[d, l, 0], pp[d, l, 1], upper, lower)
        active = flags[d, l] >= 0
        return (jnp.where(active, upper - change[:band], upper), jnp.where(active, lower - change[band:], lower))

    panels_in.wait()
    give(0)
    tiles_in.wait()
    for p in range(n_once):
        i = ordered(p, n_once, first)
        upward(0, xin.at[once0 + i + shift], u1, i).start()
    for k in (1, 2, 3):
        give(k)
    twin_panels.start()
    twin_flags.start()
    for e in range(both):
        twin_tile(e).start()
    for k in (4, 5):
        give(k)
    pass_on(0)
    flags_copy.wait()
    settle(0)
    factor_chunks(0)
    give(6)
    give(7)
    pass_on(1)
    pass_on(2)

    def early(p, carry):
        i = ordered(p, n_twice, last)
        upward(0, u1.at[i], u1, i).wait_recv()
        upper, lower = apply(0, twice0 + i, xin[twice0 + i], u1[i])
        xb[i] = upper

        @pl.when(i >= both)
        def _():
            s1[i] = lower
            downward(0, s1.at[i], d1, i).start()

        @pl.when(jnp.logical_not(first))
        def _():
            upward(1, xb.at[i], us, i).start()

        @pl.when(first & (i > 0))
        def _():
            upward(1, xb.at[i], us, i - 1).start()

        return carry

    lax.fori_loop(0, n_twice - lead, early, 0)
    pass_on(3)
    settle(1)
    settle(2)
    settle(3)
    factor_chunks(1, 2, 3)
    lax.fori_loop(n_twice - lead, n_twice, early, 0)
    pass_on(4)
    pass_on(5)
    pass_on(6)

    def middle(p, carry):
        i = n_once - 1 - p
        l = once0 + i
        closed = last & (i == n_once - 1)

        @pl.when(first & (i == 0))
        def _():
            xq[...] = xin[once0]

        j = i - shift

        @pl.when(j >= both)
        def _():
            downward(0, d1.at[j], d1, j).wait_recv()
            xq[...] = d1[j]

        @pl.when((j >= 0) & (j < both))
        def _():
            twin_tile(j).wait_recv()
            own = xin[once0 + i]
            xq[...] = own - change_of(ev[j, 0], ev[j, 1], ep[j, 0], ep[j, 1], l1[j], own)

        @pl.when(closed)
        def _():
            xc[...] = xin[once0]

        @pl.when(jnp.logical_not(closed))
        def _():
            upward(1, us.at[i], us, i).wait_recv()
            xc[...] = us[i]

        upper, lower = apply(0, l, xq[...], xc[...])
        upper, lower = apply(1, l, upper, lower)
        ss[i] = lower
        xs[i] = upper

        @pl.when(jnp.logical_not(closed))
        def _():
            downward(1, ss.at[i], ds, i).start()

        @pl.when(jnp.logical_not(first & (i == 0)))
        def _():
            upward(2, xs.at[i], u2, i - shift).start()

        return carry

    lax.fori_loop(0, 1, middle, 0)
    settle(4)
    settle(5)
    settle(6)
    twin_flags.wait_recv()
    factor_chunks(4, 5, 6)
    pass_on(7)
    @pl.when(first)
    def _():
        downward(0, d1.at[n_once - 1], d1, n_once - 1).wait_recv()
        xz[...] = jnp.where(flags[0, twice0] >= 0, xb[0], d1[n_once - 1])
        upward(2, xz, u2, n_once - 1).start()

    lax.fori_loop(1, n_once, middle, 0)

    settle(7)
    factor_chunks(7)

    def late(p, carry):
        i = ordered(p, n_twice, last)

        @pl.when(jnp.logical_not(first & (i == 0)))
        def _():
            j = i - shift
            downward(1, ds.at[j], ds, j).wait_recv()
            xc[...] = ds[j]

        @pl.when(first & (i == 0))
        def _():
            xc[...] = xz[...]

        upward(2, u2.at[i], u2, i).wait_recv()
        upper, lower = apply(1, twice0 + i, xc[...], u2[i])
        s2[i] = lower
        xf[i] = upper

        @pl.when(last & (i == n_twice - 1))
        def _():
            remote(s2.at[i], d2, dn_send.at[2], dn_recv.at[2, i], below, col).start()

        @pl.when(jnp.logical_not(last & (i == n_twice - 1)))
        def _():
            home(i, s2.at[i]).start()

        @pl.when(jnp.logical_not(first & (i == 0)))
        def _():
            pltpu.make_async_copy(xf.at[i], out.at[twice0 + i, 0], out_sem.at[0]).start()

        return carry

    lax.fori_loop(0, n_twice, late, 0)

    def left_up(kind, n):
        remote(xs.at[pl.ds(0, n)], u1.at[pl.ds(0, n)], up_send.at[kind], up_recv.at[kind, 0], above, col).wait_send()

    def left_down(kind, n):
        remote(xs.at[pl.ds(0, n)], d1.at[pl.ds(0, n)], dn_send.at[kind], dn_recv.at[kind, 0], below, col).wait_send()

    left_up(0, n_once)
    left_up(2, n_once)
    left_down(0, n_twice - both)

    @pl.when(first)
    def _():
        left_up(1, n_twice - 1)

    @pl.when(jnp.logical_not(first))
    def _():
        left_up(1, n_twice)

    @pl.when(last)
    def _():
        left_down(1, n_once - 1)

    @pl.when(jnp.logical_not(last))
    def _():
        left_down(1, n_once)

    twin_panels.wait_send()
    twin_flags.wait_send()
    for e in range(both):
        twin_tile(e).wait_send()
    departed(n_x, pan_send)

    @pl.when(core == 1)
    def _():
        departed(2 * n_x - 2, rel_send)

    @pl.when(first)
    def _():
        own = pltpu.make_async_copy(xs.at[0], out.at[once0, 0], out_sem.at[1])
        own.start()
        remote(xz, d2, dn_send.at[2], dn_recv.at[2, n_once - 1], below, col).wait_recv()
        xb[0] = jnp.where(flags[1, twice0] >= 0, xf[0], d2[...])
        pltpu.make_async_copy(xb.at[0], out.at[twice0, 0], out_sem.at[0]).start()

    def close(i, carry):
        @pl.when(jnp.logical_not(first & (i == 0)))
        def _():
            j = i - shift
            remote(s2.at[j], out.at[once0 + i, 0], dn_send.at[2], dn_recv.at[2, j], below, col).wait_recv()

        return carry

    lax.fori_loop(0, n_once, close, 0)

    left_down(2, n_twice)

    @pl.when(first)
    def _():
        pltpu.make_async_copy(xs.at[0], out.at[once0, 0], out_sem.at[1]).wait()

    pltpu.make_async_copy(xf.at[pl.ds(0, n_twice)], out.at[pl.ds(twice0, n_twice), 0], out_sem.at[0]).wait()


def local(n_row, n_x, eigvec, reflectors, sweep_group):
    tiles, _, band, width = eigvec.shape
    rows = reflectors.shape[3]
    diagonals = reflectors.shape[0]
    cap = max(FEWER, tiles - FEWER)
    one, many = pltpu.VMEM((band, width), f32), pltpu.VMEM((cap, band, width), f32)
    pair = BOTH
    dma = pltpu.SemaphoreType.DMA
    hbm = lambda array: pltpu.with_memory_space_constraint(array, pltpu.HBM)
    flags = sweep_group.reshape(sweep_group.shape[:2])
    return pl.pallas_call(
        functools.partial(kernel, n_row, n_x, FEWER),
        out_shape=jax.ShapeDtypeStruct(eigvec.shape, f32),
        in_specs=[pl.BlockSpec(memory_space=pltpu.HBM)] * 3,
        out_specs=pl.BlockSpec(memory_space=pl.ANY),
        scratch_shapes=[
            pltpu.SMEM(flags.shape, jnp.int32),
            pltpu.VMEM(flags.shape, jnp.int32),
            pltpu.VMEM((tiles, band, width), f32),
            many, many, many, one, one, one,
            many, many, many, many, many, many, many, many, one, pltpu.VMEM((pair, band, width), f32),
            pltpu.VMEM((diagonals, tiles, 2 * n_x, rows, band), f32),
            pltpu.VMEM((diagonals, tiles, 2, 2 * band, band), bf16),
            pltpu.VMEM((diagonals, tiles, 2, band, 2 * band), bf16),
            pltpu.VMEM((pair, 2 * n_x, rows, band), f32),
            pltpu.VMEM((pair, 2, band, band), bf16),
            pltpu.VMEM((pair, 2, band, 2 * band), bf16),
            dma, dma((2,)), dma((2,)), dma((pair,)), dma((pair,)),
            dma, dma, dma((2,)), dma((8,)), dma((2,)),
            dma((3,)), dma((3, cap)), dma((3,)), dma((3, cap)), dma((2,)),
        ],
        compiler_params=pltpu.CompilerParams(
            collective_id=0, has_side_effects=True, vmem_limit_bytes=48 * 1024 * 1024),
    )(hbm(eigvec), hbm(reflectors), hbm(flags))


def solution(mesh):
    return jax.shard_map(
        functools.partial(local, mesh.shape["row"], mesh.shape["col"] // 2),
        mesh=mesh,
        in_specs=(
            P(None, "row", None, "col"),
            P(None, None, "row", "col", None),
            P(None, None, "row"),
        ),
        out_specs=P(None, "row", None, "col"),
        check_vma=False,
    )
```

```python
import functools

import jax
import jax.numpy as jnp
from jax import lax
from jax.experimental import pallas as pl
from jax.experimental.pallas import tpu as pltpu
from jax.sharding import PartitionSpec as P

MESH = pl.DeviceIdType.MESH
f32, bf16 = jnp.float32, jnp.bfloat16
TILES, FEWER, BOTH = 8, 4, 1


def split(a):
    hi = a.astype(bf16)
    return hi, (a - hi.astype(f32)).astype(bf16)


def mm(a, b):
    return jnp.dot(a, b, preferred_element_type=f32)


def square_dot(a, b):
    n = a.shape[-1]
    a_hi, a_lo = split(a)
    b_hi, b_lo = split(b)
    right = jnp.concatenate([b_hi, b_lo], axis=1)
    both = mm(jnp.concatenate([a_hi, a_lo], axis=1), jnp.concatenate([right, right], axis=0))
    return both[:, :n] + both[:, n:]


def factor_panels(panels):
    depth, band = panels[0].shape
    rows = lax.broadcasted_iota(jnp.int32, (depth, band), 0)
    cols = lax.broadcasted_iota(jnp.int32, (depth, band), 1)
    inside = (rows >= cols + 1) & (rows <= cols + band)
    leading = rows == cols + 1
    r = lax.broadcasted_iota(jnp.int32, (band, band), 0)
    c = lax.broadcasted_iota(jnp.int32, (band, band), 1)
    eye, above, beside = r == c, r < c, (r + 1 == c) & (lax.rem(c, 2) == 1)
    halves, turned, factors, inverses = [], [], [], []
    coupled = above & (r // 2 != c // 2) & (r // 4 == c // 4)
    for panel in panels:
        vectors = jnp.where(leading, 1.0, jnp.where(inside, panel, 0.0))
        v_hi, v_lo = split(vectors)
        t_hi, t_lo = split(vectors.T)
        both = mm(t_hi, jnp.concatenate([v_hi, v_lo], axis=1))
        gram = both[:, :band] + both[:, band:] + mm(t_lo, v_hi)
        on_diagonal = jnp.where(eye, gram, 0.0)
        along = 2.0 / jnp.sum(on_diagonal, axis=0, keepdims=True)
        down = 2.0 / jnp.sum(on_diagonal, axis=1, keepdims=True)
        pair = jnp.where(beside, gram * along * down, 0.0)
        pair_along = -jnp.sum(pair, axis=0, keepdims=True)
        pair_down = -jnp.sum(pair, axis=1, keepdims=True)
        inverse = jnp.where(eye, along, 0.0) - pair
        upper_part = jnp.where(coupled, gram, 0.0)
        middle = upper_part * along + pltpu.roll(upper_part, 1, 1) * pair_along
        inverse = inverse - (middle * down + pltpu.roll(middle, band - 1, 0) * pair_down)
        halves.append((v_hi, v_lo))
        turned.append((t_hi, t_lo))
        factors.append(gram)
        inverses.append(inverse)
    block = 4
    while block < band:
        step = 4 if 4 * block <= band else 2
        coupling = above & (r // block != c // block) & (r // (step * block) == c // (step * block))
        if step == 2:
            middles = [square_dot(jnp.where(coupling, f, 0.0), x) for f, x in zip(factors, inverses)]
            inverses = [x - square_dot(x, m) for x, m in zip(inverses, middles)]
        else:
            moves = [square_dot(x, jnp.where(coupling, f, 0.0)) for f, x in zip(factors, inverses)]
            squares = [square_dot(m, m) for m in moves]
            firsts = [x - square_dot(m, x) for m, x in zip(moves, inverses)]
            inverses = [y + square_dot(q, y) for q, y in zip(squares, firsts)]
        block *= step
    results = []
    for (v_hi, v_lo), (t_hi, t_lo), inverse in zip(halves, turned, inverses):
        i_hi, i_lo = split(inverse)
        solver = mm(jnp.concatenate([i_hi, i_lo], axis=1), jnp.concatenate([t_hi, t_hi], axis=0)) + mm(i_hi, t_lo)
        p_hi, p_lo = split(solver)
        results.append((v_hi, v_lo, p_hi, p_lo))
    return results


def kernel(n_row, n_x, fewer, *refs):
    odd = lax.rem(lax.axis_index("row"), 2) == 1

    @pl.when(odd)
    def _():
        body(n_row, n_x, (0, fewer), (fewer, TILES - fewer), *refs)

    @pl.when(jnp.logical_not(odd))
    def _():
        body(n_row, n_x, (fewer, TILES - fewer), (0, fewer), *refs)


def body(n_row, n_x, twice, once, eig, refl, flags_in, out,
         flags, flags_above, xin, xb, xs, xf, xq, xc, xz, u1, us, u2, s1, ss, s2, d1, ds, d2, l1, pan, vv, pp, epan, ev, ep,
         flag_sem, twin_send, twin_recv, l1_send, l1_recv, in_sem, pan_in, pan_send, pan_recv, rel_send,
         up_send, up_recv, dn_send, dn_recv, out_sem):
    row = lax.axis_index("row")
    col = lax.axis_index("col")
    band = xin.shape[1]
    x, core = col // 2, lax.rem(col, 2)
    first = row == 0
    last = row == n_row - 1
    shift = jnp.where(first, 1, 0)
    next_shift = jnp.where(last, 1, 0)
    above = lax.rem(row + n_row - 1, n_row)
    below = lax.rem(row + 1, n_row)
    (twice0, n_twice), (once0, n_once) = twice, once
    partner = x * 2 + (1 - core)
    x_right, x_left, x_far = lax.rem(x + 1, n_x), lax.rem(x + n_x - 1, n_x), lax.rem(x + 2, n_x)
    right, left, far = x_right * 2 + 1, x_left * 2 + 1, x_far * 2 + 1

    both, lead = epan.shape[0], n_twice // 2
    half = n_once // 2
    chunks = ((0, twice0 + lead, n_twice - lead),
              (0, once0 + half, n_once - half), (1, once0 + half, n_once - half),
              (0, twice0, lead),
              (0, once0, half), (1, once0, half),
              None,
              (1, *twice))
    def ordered(p, n, swapped):
        return jnp.where(swapped & (p < 2), n - 2 + p, n - 1 - p)

    def shares(k, c):
        if chunks[k] is None:
            return epan.at[:, c]
        d, l0, n = chunks[k]
        return pan.at[d, pl.ds(l0, n), c]

    barrier = pltpu.get_barrier_semaphore()
    for r_, c_ in ((below, col), (above, col), (row, partner)):
        pl.semaphore_signal(barrier, inc=1, device_id=(r_, c_), device_id_type=MESH)

    @pl.when(core == 1)
    def _():
        for x_ in (x_right, x_left, x_far):
            for c_ in range(2):
                pl.semaphore_signal(barrier, inc=1, device_id=(row, x_ * 2 + c_), device_id_type=MESH)

    tiles_in = pltpu.make_async_copy(eig.at[:, 0], xin, in_sem)
    tiles_in.start()
    panels_in = pltpu.make_async_copy(refl.at[:, :, 0], pan.at[:, :, col], pan_in)
    panels_in.start()
    flags_copy = pltpu.make_async_copy(flags_in, flags, flag_sem)
    flags_copy.start()

    pl.semaphore_wait(barrier, 6)

    def remote(src, dst, ssem, rsem, r_, c_):
        return pltpu.make_async_remote_copy(src_ref=src, dst_ref=dst, send_sem=ssem, recv_sem=rsem,
                                            device_id=(r_, c_), device_id_type=MESH)

    def upward(kind, src, dst, i):
        return remote(src, dst.at[i], up_send.at[kind], up_recv.at[kind, i], above, col)

    def downward(kind, src, dst, i):
        return remote(src, dst.at[i], dn_send.at[kind], dn_recv.at[kind, i], below, col)

    def home(i, src):
        return remote(src, out.at[twice0 + next_shift + i, 0], dn_send.at[2], dn_recv.at[2, i], below, col)

    def given(k, j):
        c = shares(k, col)
        return remote(c, c, pan_send.at[1 if chunks[k] is None else 0], pan_recv.at[k], row, (right, left, far, partner)[j])

    def across(k, j, c_):
        c = shares(k, (x_left, x_right, x_far)[j] * 2 + c_)
        return remote(c, c, rel_send.at[1 if chunks[k] is None else 0], pan_recv.at[k], row, partner)

    def arrived(k):
        n = 2 * n_x - 1
        if chunks[k] is None:
            c = epan.at[:, pl.ds(0, n)]
        else:
            d, l0, m = chunks[k]
            c = pan.at[d, pl.ds(l0, m), pl.ds(0, n)]
        return remote(c, c, pan_send.at[0], pan_recv.at[k], row, partner)

    def departed(n, send_sem):
        own, other = pan.at[:, :, pl.ds(0, n)], epan.at[:, pl.ds(0, n)]
        remote(own, own, send_sem.at[0], pan_recv.at[0], row, partner).wait_send()
        remote(other, other, send_sem.at[1], pan_recv.at[0], row, partner).wait_send()

    arrivals = [(j, c_) for j in range(3) for c_ in (1, 0)]

    twin_panels = remote(pan.at[0, pl.ds(twice0, both), col], epan.at[:, col], twin_send.at[0], twin_recv.at[0], below, col)
    twin_flags = remote(flags_in, flags_above, twin_send.at[1], twin_recv.at[1], below, col)

    def twin_tile(e):
        return remote(xin.at[twice0 + e], l1.at[e], l1_send.at[e], l1_recv.at[e], below, col)

    def give(k):
        if chunks[k] is None:
            twin_panels.wait_recv()
        for j in (3, 2, 0, 1):
            given(k, j).start()

    def pass_on(k):
        @pl.when(core == 1)
        def _():
            arrived(k).wait_recv()
            for j, c_ in arrivals:
                across(k, j, c_).start()

    def settle(k):
        @pl.when(core == 0)
        def _():
            arrived(k).wait_recv()

    def factor_chunks(*ks):
        with_above = any(chunks[k] is None for k in ks)
        at = [(chunks[k][0], chunks[k][1] + i) for k in ks if chunks[k] for i in range(chunks[k][2])]
        raw = [pan[d, l].reshape(2 * band, band) for d, l in at]
        if with_above:
            raw += [epan[e].reshape(2 * band, band) for e in range(both)]
        results = factor_panels(raw)
        for (d, l), (v_hi, v_lo, p_hi, p_lo) in zip(at, results):
            vv[d, l, 0] = v_hi
            vv[d, l, 1] = v_lo
            pp[d, l, 0] = p_hi
            pp[d, l, 1] = p_lo

        if with_above:
            for e, (v_hi, v_lo, p_hi, p_lo) in enumerate(results[len(at):]):
                present = flags_above[0:1, once0 + e:once0 + e + 1] >= 0
                ev[e, 0] = v_hi[band:]
                ev[e, 1] = v_lo[band:]
                ep[e, 0] = jnp.where(present, p_hi.astype(f32), 0.0).astype(bf16)
                ep[e, 1] = jnp.where(present, p_lo.astype(f32), 0.0).astype(bf16)

    def change_of(v_hi, v_lo, p_hi, p_lo, upper, lower):
        s_hi, s_lo = split(jnp.concatenate([upper, lower], axis=0))
        w_hi, w_lo = split(mm(p_hi, s_hi) + mm(p_hi, s_lo) + mm(p_lo, s_hi))
        return mm(jnp.concatenate([v_hi, v_lo], axis=1), jnp.concatenate([w_hi, w_hi], axis=0)) + mm(v_hi, w_lo)

    def apply(d, l, upper, lower):
        change = change_of(vv[d, l, 0], vv[d, l, 1], pp[d, l, 0], pp[d, l, 1], upper, lower)
        active = flags[d, l] >= 0
        return (jnp.where(active, upper - change[:band], upper), jnp.where(active, lower - change[band:], lower))

    tiles_in.wait()
    for p in range(n_once):
        i = ordered(p, n_once, first)
        upward(0, xin.at[once0 + i + shift], u1, i).start()
    panels_in.wait()
    give(0)
    for k in (1, 2, 3):
        give(k)
    twin_panels.start()
    twin_flags.start()
    for e in range(both):
        twin_tile(e).start()
    for k in (4, 5):
        give(k)
    pass_on(0)
    flags_copy.wait()
    settle(0)
    factor_chunks(0)
    give(6)
    give(7)
    pass_on(1)
    pass_on(2)

    def early(p, carry):
        i = ordered(p, n_twice, last)
        upward(0, u1.at[i], u1, i).wait_recv()
        upper, lower = apply(0, twice0 + i, xin[twice0 + i], u1[i])
        xb[i] = upper

        @pl.when(i >= both)
        def _():
            s1[i] = lower
            downward(0, s1.at[i], d1, i).start()

        @pl.when(jnp.logical_not(first))
        def _():
            upward(1, xb.at[i], us, i).start()

        @pl.when(first & (i > 0))
        def _():
            upward(1, xb.at[i], us, i - 1).start()

        return carry

    lax.fori_loop(0, n_twice - lead, early, 0)
    pass_on(3)
    settle(1)
    settle(2)
    settle(3)
    factor_chunks(1, 2, 3)
    lax.fori_loop(n_twice - lead, n_twice, early, 0)
    pass_on(4)
    pass_on(5)
    pass_on(6)

    def middle(p, carry):
        i = n_once - 1 - p
        l = once0 + i
        closed = last & (i == n_once - 1)

        @pl.when(first & (i == 0))
        def _():
            xq[...] = xin[once0]

        j = i - shift

        @pl.when(j >= both)
        def _():
            downward(0, d1.at[j], d1, j).wait_recv()
            xq[...] = d1[j]

        @pl.when((j >= 0) & (j < both))
        def _():
            twin_tile(j).wait_recv()
            own = xin[once0 + i]
            xq[...] = own - change_of(ev[j, 0], ev[j, 1], ep[j, 0], ep[j, 1], l1[j], own)

        @pl.when(closed)
        def _():
            xc[...] = xin[once0]

        @pl.when(jnp.logical_not(closed))
        def _():
            upward(1, us.at[i], us, i).wait_recv()
            xc[...] = us[i]

        upper, lower = apply(0, l, xq[...], xc[...])
        upper, lower = apply(1, l, upper, lower)
        ss[i] = lower
        xs[i] = upper

        @pl.when(jnp.logical_not(closed))
        def _():
            downward(1, ss.at[i], ds, i).start()

        @pl.when(jnp.logical_not(first & (i == 0)))
        def _():
            upward(2, xs.at[i], u2, i - shift).start()

        return carry

    lax.fori_loop(0, 1, middle, 0)
    settle(4)
    settle(5)
    settle(6)
    twin_flags.wait_recv()
    factor_chunks(4, 5, 6)
    pass_on(7)
    @pl.when(first)
    def _():
        downward(0, d1.at[n_once - 1], d1, n_once - 1).wait_recv()
        xz[...] = jnp.where(flags[0, twice0] >= 0, xb[0], d1[n_once - 1])
        upward(2, xz, u2, n_once - 1).start()

    lax.fori_loop(1, n_once, middle, 0)

    settle(7)
    factor_chunks(7)

    def late(p, carry):
        i = ordered(p, n_twice, last)

        @pl.when(jnp.logical_not(first & (i == 0)))
        def _():
            j = i - shift
            downward(1, ds.at[j], ds, j).wait_recv()
            xc[...] = ds[j]

        @pl.when(first & (i == 0))
        def _():
            xc[...] = xz[...]

        upward(2, u2.at[i], u2, i).wait_recv()
        upper, lower = apply(1, twice0 + i, xc[...], u2[i])
        s2[i] = lower
        xf[i] = upper

        @pl.when(last & (i == n_twice - 1))
        def _():
            remote(s2.at[i], d2, dn_send.at[2], dn_recv.at[2, i], below, col).start()

        @pl.when(jnp.logical_not(last & (i == n_twice - 1)))
        def _():
            home(i, s2.at[i]).start()

        @pl.when(jnp.logical_not(first & (i == 0)))
        def _():
            pltpu.make_async_copy(xf.at[i], out.at[twice0 + i, 0], out_sem.at[0]).start()

        return carry

    lax.fori_loop(0, n_twice, late, 0)

    def left_up(kind, n):
        remote(xs.at[pl.ds(0, n)], u1.at[pl.ds(0, n)], up_send.at[kind], up_recv.at[kind, 0], above, col).wait_send()

    def left_down(kind, n):
        remote(xs.at[pl.ds(0, n)], d1.at[pl.ds(0, n)], dn_send.at[kind], dn_recv.at[kind, 0], below, col).wait_send()

    left_up(0, n_once)
    left_up(2, n_once)
    left_down(0, n_twice - both)

    @pl.when(first)
    def _():
        left_up(1, n_twice - 1)

    @pl.when(jnp.logical_not(first))
    def _():
        left_up(1, n_twice)

    @pl.when(last)
    def _():
        left_down(1, n_once - 1)

    @pl.when(jnp.logical_not(last))
    def _():
        left_down(1, n_once)

    twin_panels.wait_send()
    twin_flags.wait_send()
    for e in range(both):
        twin_tile(e).wait_send()
    departed(n_x, pan_send)

    @pl.when(core == 1)
    def _():
        departed(2 * n_x - 2, rel_send)

    @pl.when(first)
    def _():
        own = pltpu.make_async_copy(xs.at[0], out.at[once0, 0], out_sem.at[1])
        own.start()
        remote(xz, d2, dn_send.at[2], dn_recv.at[2, n_once - 1], below, col).wait_recv()
        xb[0] = jnp.where(flags[1, twice0] >= 0, xf[0], d2[...])
        pltpu.make_async_copy(xb.at[0], out.at[twice0, 0], out_sem.at[0]).start()

    def close(i, carry):
        @pl.when(jnp.logical_not(first & (i == 0)))
        def _():
            j = i - shift
            remote(s2.at[j], out.at[once0 + i, 0], dn_send.at[2], dn_recv.at[2, j], below, col).wait_recv()

        return carry

    lax.fori_loop(0, n_once, close, 0)

    left_down(2, n_twice)

    @pl.when(first)
    def _():
        pltpu.make_async_copy(xs.at[0], out.at[once0, 0], out_sem.at[1]).wait()

    pltpu.make_async_copy(xf.at[pl.ds(0, n_twice)], out.at[pl.ds(twice0, n_twice), 0], out_sem.at[0]).wait()


def local(n_row, n_x, eigvec, reflectors, sweep_group):
    tiles, _, band, width = eigvec.shape
    rows = reflectors.shape[3]
    diagonals = reflectors.shape[0]
    cap = max(FEWER, tiles - FEWER)
    one, many = pltpu.VMEM((band, width), f32), pltpu.VMEM((cap, band, width), f32)
    pair = BOTH
    dma = pltpu.SemaphoreType.DMA
    hbm = lambda array: pltpu.with_memory_space_constraint(array, pltpu.HBM)
    flags = sweep_group.reshape(sweep_group.shape[:2])
    return pl.pallas_call(
        functools.partial(kernel, n_row, n_x, FEWER),
        out_shape=jax.ShapeDtypeStruct(eigvec.shape, f32),
        in_specs=[pl.BlockSpec(memory_space=pltpu.HBM)] * 3,
        out_specs=pl.BlockSpec(memory_space=pl.ANY),
        scratch_shapes=[
            pltpu.SMEM(flags.shape, jnp.int32),
            pltpu.VMEM(flags.shape, jnp.int32),
            pltpu.VMEM((tiles, band, width), f32),
            many, many, many, one, one, one,
            many, many, many, many, many, many, many, many, one, pltpu.VMEM((pair, band, width), f32),
            pltpu.VMEM((diagonals, tiles, 2 * n_x, rows, band), f32),
            pltpu.VMEM((diagonals, tiles, 2, 2 * band, band), bf16),
            pltpu.VMEM((diagonals, tiles, 2, band, 2 * band), bf16),
            pltpu.VMEM((pair, 2 * n_x, rows, band), f32),
            pltpu.VMEM((pair, 2, band, band), bf16),
            pltpu.VMEM((pair, 2, band, 2 * band), bf16),
            dma, dma((2,)), dma((2,)), dma((pair,)), dma((pair,)),
            dma, dma, dma((2,)), dma((8,)), dma((2,)),
            dma((3,)), dma((3, cap)), dma((3,)), dma((3, cap)), dma((2,)),
        ],
        compiler_params=pltpu.CompilerParams(
            collective_id=0, has_side_effects=True, vmem_limit_bytes=48 * 1024 * 1024),
    )(hbm(eigvec), hbm(reflectors), hbm(flags))


def solution(mesh):
    return jax.shard_map(
        functools.partial(local, mesh.shape["row"], mesh.shape["col"] // 2),
        mesh=mesh,
        in_specs=(
            P(None, "row", None, "col"),
            P(None, None, "row", "col", None),
            P(None, None, "row"),
        ),
        out_specs=P(None, "row", None, "col"),
        check_vma=False,
    )
```

```python
import functools

import jax
import jax.numpy as jnp
from jax import lax
from jax.experimental import pallas as pl
from jax.experimental.pallas import tpu as pltpu
from jax.sharding import PartitionSpec as P

MESH = pl.DeviceIdType.MESH
f32, bf16 = jnp.float32, jnp.bfloat16
TILES, FEWER, BOTH = 8, 4, 1


def split(a):
    hi = a.astype(bf16)
    return hi, (a - hi.astype(f32)).astype(bf16)


def mm(a, b):
    return jnp.dot(a, b, preferred_element_type=f32)


def square_dot(a, b):
    n = a.shape[-1]
    a_hi, a_lo = split(a)
    b_hi, b_lo = split(b)
    right = jnp.concatenate([b_hi, b_lo], axis=1)
    both = mm(jnp.concatenate([a_hi, a_lo], axis=1), jnp.concatenate([right, right], axis=0))
    return both[:, :n] + both[:, n:]


def factor_panels(panels):
    depth, band = panels[0].shape
    rows = lax.broadcasted_iota(jnp.int32, (depth, band), 0)
    cols = lax.broadcasted_iota(jnp.int32, (depth, band), 1)
    inside = (rows >= cols + 1) & (rows <= cols + band)
    leading = rows == cols + 1
    r = lax.broadcasted_iota(jnp.int32, (band, band), 0)
    c = lax.broadcasted_iota(jnp.int32, (band, band), 1)
    eye, above, beside = r == c, r < c, (r + 1 == c) & (lax.rem(c, 2) == 1)
    halves, turned, factors, inverses = [], [], [], []
    coupled = above & (r // 2 != c // 2) & (r // 4 == c // 4)
    for panel in panels:
        vectors = jnp.where(leading, 1.0, jnp.where(inside, panel, 0.0))
        v_hi, v_lo = split(vectors)
        t_hi, t_lo = split(vectors.T)
        both = mm(t_hi, jnp.concatenate([v_hi, v_lo], axis=1))
        gram = both[:, :band] + both[:, band:] + mm(t_lo, v_hi)
        on_diagonal = jnp.where(eye, gram, 0.0)
        along = 2.0 / jnp.sum(on_diagonal, axis=0, keepdims=True)
        down = 2.0 / jnp.sum(on_diagonal, axis=1, keepdims=True)
        pair = jnp.where(beside, gram * along * down, 0.0)
        pair_along = -jnp.sum(pair, axis=0, keepdims=True)
        pair_down = -jnp.sum(pair, axis=1, keepdims=True)
        inverse = jnp.where(eye, along, 0.0) - pair
        upper_part = jnp.where(coupled, gram, 0.0)
        middle = upper_part * along + pltpu.roll(upper_part, 1, 1) * pair_along
        inverse = inverse - (middle * down + pltpu.roll(middle, band - 1, 0) * pair_down)
        halves.append((v_hi, v_lo))
        turned.append((t_hi, t_lo))
        factors.append(gram)
        inverses.append(inverse)
    block = 4
    while block < band:
        step = 4 if 4 * block <= band else 2
        coupling = above & (r // block != c // block) & (r // (step * block) == c // (step * block))
        if step == 2:
            middles = [square_dot(jnp.where(coupling, f, 0.0), x) for f, x in zip(factors, inverses)]
            inverses = [x - square_dot(x, m) for x, m in zip(inverses, middles)]
        else:
            moves = [square_dot(x, jnp.where(coupling, f, 0.0)) for f, x in zip(factors, inverses)]
            squares = [square_dot(m, m) for m in moves]
            firsts = [x - square_dot(m, x) for m, x in zip(moves, inverses)]
            inverses = [y + square_dot(q, y) for q, y in zip(squares, firsts)]
        block *= step
    results = []
    for (v_hi, v_lo), (t_hi, t_lo), inverse in zip(halves, turned, inverses):
        i_hi, i_lo = split(inverse)
        solver = mm(jnp.concatenate([i_hi, i_lo], axis=1), jnp.concatenate([t_hi, t_hi], axis=0)) + mm(i_hi, t_lo)
        p_hi, p_lo = split(solver)
        results.append((v_hi, v_lo, p_hi, p_lo))
    return results


def kernel(n_row, n_x, fewer, *refs):
    odd = lax.rem(lax.axis_index("row"), 2) == 1

    @pl.when(odd)
    def _():
        body(n_row, n_x, (0, fewer), (fewer, TILES - fewer), *refs)

    @pl.when(jnp.logical_not(odd))
    def _():
        body(n_row, n_x, (fewer, TILES - fewer), (0, fewer), *refs)


def body(n_row, n_x, twice, once, eig, refl, flags_in, out,
         flags, flags_above, xin, xb, xs, xf, xq, xc, xz, u1, us, u2, s1, ss, s2, d1, ds, d2, l1, pan, vv, pp, epan, ev, ep,
         flag_sem, twin_send, twin_recv, l1_send, l1_recv, in_sem, pan_in, pan_send, pan_recv, rel_send,
         up_send, up_recv, dn_send, dn_recv, out_sem):
    row = lax.axis_index("row")
    col = lax.axis_index("col")
    band = xin.shape[1]
    x, core = col // 2, lax.rem(col, 2)
    first = row == 0
    last = row == n_row - 1
    shift = jnp.where(first, 1, 0)
    next_shift = jnp.where(last, 1, 0)
    above = lax.rem(row + n_row - 1, n_row)
    below = lax.rem(row + 1, n_row)
    (twice0, n_twice), (once0, n_once) = twice, once
    partner = x * 2 + (1 - core)
    x_right, x_left, x_far = lax.rem(x + 1, n_x), lax.rem(x + n_x - 1, n_x), lax.rem(x + 2, n_x)
    right, left, far = x_right * 2 + 1, x_left * 2 + 1, x_far * 2 + 1

    both, lead = epan.shape[0], n_twice // 2
    half = n_once // 2
    chunks = ((0, twice0 + lead, n_twice - lead),
              (0, once0 + half, n_once - half), (1, once0 + half, n_once - half),
              (0, twice0, lead),
              (0, once0, half), (1, once0, half),
              None,
              (1, *twice))
    def ordered(p, n, swapped):
        return jnp.where(swapped & (p < 2), n - 2 + p, n - 1 - p)

    def shares(k, c):
        if chunks[k] is None:
            return epan.at[:, c]
        d, l0, n = chunks[k]
        return pan.at[d, pl.ds(l0, n), c]

    barrier = pltpu.get_barrier_semaphore()
    for r_, c_ in ((below, col), (above, col), (row, partner)):
        pl.semaphore_signal(barrier, inc=1, device_id=(r_, c_), device_id_type=MESH)

    @pl.when(core == 1)
    def _():
        for x_ in (x_right, x_left, x_far):
            for c_ in range(2):
                pl.semaphore_signal(barrier, inc=1, device_id=(row, x_ * 2 + c_), device_id_type=MESH)

    tiles_in = pltpu.make_async_copy(eig.at[:, 0], xin, in_sem)
    tiles_in.start()
    panels_in = pltpu.make_async_copy(refl.at[:, :, 0], pan.at[:, :, col], pan_in)
    panels_in.start()
    flags_copy = pltpu.make_async_copy(flags_in, flags, flag_sem)
    flags_copy.start()

    pl.semaphore_wait(barrier, 6)

    def remote(src, dst, ssem, rsem, r_, c_):
        return pltpu.make_async_remote_copy(src_ref=src, dst_ref=dst, send_sem=ssem, recv_sem=rsem,
                                            device_id=(r_, c_), device_id_type=MESH)

    def upward(kind, src, dst, i):
        return remote(src, dst.at[i], up_send.at[kind], up_recv.at[kind, i], above, col)

    def downward(kind, src, dst, i):
        return remote(src, dst.at[i], dn_send.at[kind], dn_recv.at[kind, i], below, col)

    def home(i, src):
        return remote(src, out.at[twice0 + next_shift + i, 0], dn_send.at[2], dn_recv.at[2, i], below, col)

    def given(k, j):
        c = shares(k, col)
        return remote(c, c, pan_send.at[1 if chunks[k] is None else 0], pan_recv.at[k], row, (right, left, far, partner)[j])

    def across(k, j, c_):
        c = shares(k, (x_left, x_right, x_far)[j] * 2 + c_)
        return remote(c, c, rel_send.at[1 if chunks[k] is None else 0], pan_recv.at[k], row, partner)

    def arrived(k):
        n = 2 * n_x - 1
        if chunks[k] is None:
            c = epan.at[:, pl.ds(0, n)]
        else:
            d, l0, m = chunks[k]
            c = pan.at[d, pl.ds(l0, m), pl.ds(0, n)]
        return remote(c, c, pan_send.at[0], pan_recv.at[k], row, partner)

    def departed(n, send_sem):
        own, other = pan.at[:, :, pl.ds(0, n)], epan.at[:, pl.ds(0, n)]
        remote(own, own, send_sem.at[0], pan_recv.at[0], row, partner).wait_send()
        remote(other, other, send_sem.at[1], pan_recv.at[0], row, partner).wait_send()

    arrivals = [(j, c_) for j in range(3) for c_ in (1, 0)]

    twin_panels = remote(pan.at[0, pl.ds(twice0, both), col], epan.at[:, col], twin_send.at[0], twin_recv.at[0], below, col)
    twin_flags = remote(flags_in, flags_above, twin_send.at[1], twin_recv.at[1], below, col)

    def twin_tile(e):
        return remote(xin.at[twice0 + e], l1.at[e], l1_send.at[e], l1_recv.at[e], below, col)

    def give(k):
        if chunks[k] is None:
            twin_panels.wait_recv()
        for j in (3, 2, 0, 1):
            given(k, j).start()

    def pass_on(k):
        @pl.when(core == 1)
        def _():
            arrived(k).wait_recv()
            for j, c_ in arrivals:
                across(k, j, c_).start()

    def settle(k):
        @pl.when(core == 0)
        def _():
            arrived(k).wait_recv()

    def factor_chunks(*ks):
        with_above = any(chunks[k] is None for k in ks)
        at = [(chunks[k][0], chunks[k][1] + i) for k in ks if chunks[k] for i in range(chunks[k][2])]
        raw = [pan[d, l].reshape(2 * band, band) for d, l in at]
        if with_above:
            raw += [epan[e].reshape(2 * band, band) for e in range(both)]
        results = factor_panels(raw)
        for (d, l), (v_hi, v_lo, p_hi, p_lo) in zip(at, results):
            vv[d, l, 0] = v_hi
            vv[d, l, 1] = v_lo
            pp[d, l, 0] = p_hi
            pp[d, l, 1] = p_lo

        if with_above:
            for e, (v_hi, v_lo, p_hi, p_lo) in enumerate(results[len(at):]):
                present = flags_above[0:1, once0 + e:once0 + e + 1] >= 0
                ev[e, 0] = v_hi[band:]
                ev[e, 1] = v_lo[band:]
                ep[e, 0] = jnp.where(present, p_hi.astype(f32), 0.0).astype(bf16)
                ep[e, 1] = jnp.where(present, p_lo.astype(f32), 0.0).astype(bf16)

    def change_of(v_hi, v_lo, p_hi, p_lo, upper, lower):
        s_hi, s_lo = split(jnp.concatenate([upper, lower], axis=0))
        w_hi, w_lo = split(mm(p_hi, s_hi) + mm(p_hi, s_lo) + mm(p_lo, s_hi))
        return mm(jnp.concatenate([v_hi, v_lo], axis=1), jnp.concatenate([w_hi, w_hi], axis=0)) + mm(v_hi, w_lo)

    def apply(d, l, upper, lower):
        change = change_of(vv[d, l, 0], vv[d, l, 1], pp[d, l, 0], pp[d, l, 1], upper, lower)
        active = flags[d, l] >= 0
        return (jnp.where(active, upper - change[:band], upper), jnp.where(active, lower - change[band:], lower))

    tiles_in.wait()
    for p in range(n_once):
        i = ordered(p, n_once, first)
        upward(0, xin.at[once0 + i + shift], u1, i).start()
    panels_in.wait()
    give(0)
    for k in (1, 2, 3):
        give(k)
    twin_panels.start()
    twin_flags.start()
    for e in range(both):
        twin_tile(e).start()
    for k in (4, 5):
        give(k)
    pass_on(0)
    flags_copy.wait()
    settle(0)
    factor_chunks(0)
    give(6)
    give(7)
    pass_on(1)
    pass_on(2)

    def early(p, carry):
        i = ordered(p, n_twice, last)
        upward(0, u1.at[i], u1, i).wait_recv()
        upper, lower = apply(0, twice0 + i, xin[twice0 + i], u1[i])
        xb[i] = upper

        @pl.when(i >= both)
        def _():
            s1[i] = lower
            downward(0, s1.at[i], d1, i).start()

        @pl.when(jnp.logical_not(first))
        def _():
            upward(1, xb.at[i], us, i).start()

        @pl.when(first & (i > 0))
        def _():
            upward(1, xb.at[i], us, i - 1).start()

        return carry

    lax.fori_loop(0, n_twice - lead, early, 0)
    pass_on(3)
    settle(1)
    settle(2)
    settle(3)
    factor_chunks(1, 2, 3)
    lax.fori_loop(n_twice - lead, n_twice, early, 0)
    pass_on(4)
    pass_on(5)
    pass_on(6)

    def middle(p, carry):
        i = n_once - 1 - p
        l = once0 + i
        closed = last & (i == n_once - 1)

        @pl.when(first & (i == 0))
        def _():
            xq[...] = xin[once0]

        j = i - shift

        @pl.when(j >= both)
        def _():
            downward(0, d1.at[j], d1, j).wait_recv()
            xq[...] = d1[j]

        @pl.when((j >= 0) & (j < both))
        def _():
            twin_tile(j).wait_recv()
            own = xin[once0 + i]
            xq[...] = own - change_of(ev[j, 0], ev[j, 1], ep[j, 0], ep[j, 1], l1[j], own)

        @pl.when(closed)
        def _():
            xc[...] = xin[once0]

        @pl.when(jnp.logical_not(closed))
        def _():
            upward(1, us.at[i], us, i).wait_recv()
            xc[...] = us[i]

        upper, lower = apply(0, l, xq[...], xc[...])
        upper, lower = apply(1, l, upper, lower)
        ss[i] = lower
        xs[i] = upper

        @pl.when(jnp.logical_not(closed))
        def _():
            downward(1, ss.at[i], ds, i).start()

        @pl.when(jnp.logical_not(first & (i == 0)))
        def _():
            upward(2, xs.at[i], u2, i - shift).start()

        return carry

    ahead = jnp.where(last, 2, 1)
    lax.fori_loop(0, ahead, middle, 0)
    settle(4)
    settle(5)
    settle(6)
    twin_flags.wait_recv()
    factor_chunks(4, 5, 6)
    pass_on(7)
    @pl.when(first)
    def _():
        downward(0, d1.at[n_once - 1], d1, n_once - 1).wait_recv()
        xz[...] = jnp.where(flags[0, twice0] >= 0, xb[0], d1[n_once - 1])
        upward(2, xz, u2, n_once - 1).start()

    lax.fori_loop(ahead, n_once, middle, 0)

    settle(7)
    factor_chunks(7)

    def late(p, carry):
        i = ordered(p, n_twice, last)

        @pl.when(jnp.logical_not(first & (i == 0)))
        def _():
            j = i - shift
            downward(1, ds.at[j], ds, j).wait_recv()
            xc[...] = ds[j]

        @pl.when(first & (i == 0))
        def _():
            xc[...] = xz[...]

        upward(2, u2.at[i], u2, i).wait_recv()
        upper, lower = apply(1, twice0 + i, xc[...], u2[i])
        s2[i] = lower
        xf[i] = upper

        @pl.when(last & (i == n_twice - 1))
        def _():
            remote(s2.at[i], d2, dn_send.at[2], dn_recv.at[2, i], below, col).start()

        @pl.when(jnp.logical_not(last & (i == n_twice - 1)))
        def _():
            home(i, s2.at[i]).start()

        @pl.when(jnp.logical_not(first & (i == 0)))
        def _():
            pltpu.make_async_copy(xf.at[i], out.at[twice0 + i, 0], out_sem.at[0]).start()

        return carry

    lax.fori_loop(0, n_twice, late, 0)

    def left_up(kind, n):
        remote(xs.at[pl.ds(0, n)], u1.at[pl.ds(0, n)], up_send.at[kind], up_recv.at[kind, 0], above, col).wait_send()

    def left_down(kind, n):
        remote(xs.at[pl.ds(0, n)], d1.at[pl.ds(0, n)], dn_send.at[kind], dn_recv.at[kind, 0], below, col).wait_send()

    left_up(0, n_once)
    left_up(2, n_once)
    left_down(0, n_twice - both)

    @pl.when(first)
    def _():
        left_up(1, n_twice - 1)

    @pl.when(jnp.logical_not(first))
    def _():
        left_up(1, n_twice)

    @pl.when(last)
    def _():
        left_down(1, n_once - 1)

    @pl.when(jnp.logical_not(last))
    def _():
        left_down(1, n_once)

    twin_panels.wait_send()
    twin_flags.wait_send()
    for e in range(both):
        twin_tile(e).wait_send()
    departed(n_x, pan_send)

    @pl.when(core == 1)
    def _():
        departed(2 * n_x - 2, rel_send)

    @pl.when(first)
    def _():
        own = pltpu.make_async_copy(xs.at[0], out.at[once0, 0], out_sem.at[1])
        own.start()
        remote(xz, d2, dn_send.at[2], dn_recv.at[2, n_once - 1], below, col).wait_recv()
        xb[0] = jnp.where(flags[1, twice0] >= 0, xf[0], d2[...])
        pltpu.make_async_copy(xb.at[0], out.at[twice0, 0], out_sem.at[0]).start()

    def close(i, carry):
        @pl.when(jnp.logical_not(first & (i == 0)))
        def _():
            j = i - shift
            remote(s2.at[j], out.at[once0 + i, 0], dn_send.at[2], dn_recv.at[2, j], below, col).wait_recv()

        return carry

    lax.fori_loop(0, n_once, close, 0)

    left_down(2, n_twice)

    @pl.when(first)
    def _():
        pltpu.make_async_copy(xs.at[0], out.at[once0, 0], out_sem.at[1]).wait()

    pltpu.make_async_copy(xf.at[pl.ds(0, n_twice)], out.at[pl.ds(twice0, n_twice), 0], out_sem.at[0]).wait()


def local(n_row, n_x, eigvec, reflectors, sweep_group):
    tiles, _, band, width = eigvec.shape
    rows = reflectors.shape[3]
    diagonals = reflectors.shape[0]
    cap = max(FEWER, tiles - FEWER)
    one, many = pltpu.VMEM((band, width), f32), pltpu.VMEM((cap, band, width), f32)
    pair = BOTH
    dma = pltpu.SemaphoreType.DMA
    hbm = lambda array: pltpu.with_memory_space_constraint(array, pltpu.HBM)
    flags = sweep_group.reshape(sweep_group.shape[:2])
    return pl.pallas_call(
        functools.partial(kernel, n_row, n_x, FEWER),
        out_shape=jax.ShapeDtypeStruct(eigvec.shape, f32),
        in_specs=[pl.BlockSpec(memory_space=pltpu.HBM)] * 3,
        out_specs=pl.BlockSpec(memory_space=pl.ANY),
        scratch_shapes=[
            pltpu.SMEM(flags.shape, jnp.int32),
            pltpu.VMEM(flags.shape, jnp.int32),
            pltpu.VMEM((tiles, band, width), f32),
            many, many, many, one, one, one,
            many, many, many, many, many, many, many, many, one, pltpu.VMEM((pair, band, width), f32),
            pltpu.VMEM((diagonals, tiles, 2 * n_x, rows, band), f32),
            pltpu.VMEM((diagonals, tiles, 2, 2 * band, band), bf16),
            pltpu.VMEM((diagonals, tiles, 2, band, 2 * band), bf16),
            pltpu.VMEM((pair, 2 * n_x, rows, band), f32),
            pltpu.VMEM((pair, 2, band, band), bf16),
            pltpu.VMEM((pair, 2, band, 2 * band), bf16),
            dma, dma((2,)), dma((2,)), dma((pair,)), dma((pair,)),
            dma, dma, dma((2,)), dma((8,)), dma((2,)),
            dma((3,)), dma((3, cap)), dma((3,)), dma((3, cap)), dma((2,)),
        ],
        compiler_params=pltpu.CompilerParams(
            collective_id=0, has_side_effects=True, vmem_limit_bytes=48 * 1024 * 1024),
    )(hbm(eigvec), hbm(reflectors), hbm(flags))


def solution(mesh):
    return jax.shard_map(
        functools.partial(local, mesh.shape["row"], mesh.shape["col"] // 2),
        mesh=mesh,
        in_specs=(
            P(None, "row", None, "col"),
            P(None, None, "row", "col", None),
            P(None, None, "row"),
        ),
        out_specs=P(None, "row", None, "col"),
        check_vma=False,
    )
```
